32 devices in a mesh: grp: 4 (over y, core), peer: 8 (over z, x).
Axes of the slice: x: 2, y: 2, z: 4, core: 2. Of those that a mesh axis runs over, the one named last changes fastest.
Arguments:
- nodes: bfloat16 [65536, 64], P(('grp', 'peer')), may hold values from -6 to 6
- edges: bfloat16 [1048576, 64], P(('grp', 'peer')), may hold values from -6 to 6
- send_nodes: int32 [1048576], P(('grp', 'peer')), may hold values from 0 to 2047
- block_tile: int32 [8192], P(('grp', 'peer')), may hold values from 0 to 15
- block_count: int32 [8192], P(('grp', 'peer')), may hold values from 1 to 128, 629145 in all
- slot_ids: int32 [1048576], P(('grp', 'peer')), may hold values from 0 to 127
- edge_in_weight: bfloat16 [192, 64], replicated, may hold values from -0.4375 to 0.4375
- edge_in_bias: float32 [64], replicated, may hold values from -3 to 3
- edge_out_weight: bfloat16 [64, 64], replicated, may hold values from -0.75 to 0.75
- edge_out_bias: float32 [64], replicated, may hold values from -3 to 3
- edge_gain: float32 [64], replicated, may hold values from 0.5 to 1.5
- edge_shift: float32 [64], replicated, may hold values from -3 to 3
- node_in_weight: bfloat16 [128, 64], replicated, may hold values from -0.5 to 0.5
- node_in_bias: float32 [64], replicated, may hold values from -3 to 3
- node_out_weight: bfloat16 [64, 64], replicated, may hold values from -0.75 to 0.75
- node_out_bias: float32 [64], replicated, may hold values from -3 to 3
- node_gain: float32 [64], replicated, may hold values from 0.5 to 1.5
- node_shift: float32 [64], replicated, may hold values from -3 to 3
- node_cot: bfloat16 [65536, 64], P(('grp', 'peer')), may hold values from -6 to 6
- edge_cot: bfloat16 [1048576, 64], P(('grp', 'peer')), may hold values from -6 to 6
Outputs:
- node_result: bfloat16 [65536, 64], P(('grp', 'peer'))
- edge_result: bfloat16 [1048576, 64], P(('grp', 'peer'))
- node_grad: float32 [65536, 64], P(('grp', 'peer'))
- edge_grad: float32 [1048576, 64], P(('grp', 'peer'))
- edge_in_weight_grad: float32 [192, 64], replicated
- edge_in_bias_grad: float32 [64], replicated
- edge_out_weight_grad: float32 [64, 64], replicated
- edge_out_bias_grad: float32 [64], replicated
- edge_gain_grad: float32 [64], replicated
- edge_shift_grad: float32 [64], replicated
- node_in_weight_grad: float32 [128, 64], replicated
- node_in_bias_grad: float32 [64], replicated
- node_out_weight_grad: float32 [64, 64], replicated
- node_out_bias_grad: float32 [64], replicated
- node_gain_grad: float32 [64], replicated
- node_shift_grad: float32 [64], replicated
The draws below stay inside these ranges and needn't reach their ends.
Inputs may be any that keep to these rules, and one draw needn't show every extreme that they name: `block_tile`: tile of 128 receivers among the owner's 16.
All inputs are finite; a program needn't handle non-finite values. No bound on the sum of `block_count` on one device may be relied on, other than what follows from the above.
Results may differ from the reference program's by a relative error of at most 0.0094.
Values may be sent and summed in bfloat16 or wider, within the bound.
No kernel may reach another device: no remote copies, remote signals or barrier semaphores. Data moves between devices by JAX's collectives and lax.ppermute only.
A program may use at most 192 MiB of HBM per device.

```python
import math
import jax
import jax.numpy as jnp
import numpy as np
from jax import lax

D = 64
BLOCK = 128
TILES_DEV = 16
BLOCKS_DEV = 256
NODE_DEV = 2048
PEER_BLOCKS = 32
NODES = 65536
NBLOCKS = 8192
SLOTS = 1048576
N_GRP = 4
N_PEER = 8


def set_ends(result, own_key, low, largest):
    extent = result.shape
    index_at = [jax.random.randint(jax.random.fold_in(own_key, axis), (), 0, extent[axis]) for axis in range(len(extent))]
    result = result.at[tuple(index_at)].set(low)
    longest = extent.index(max(extent))
    index_at[longest] = (index_at[longest] + 1) % extent[longest]
    return result.at[tuple(index_at)].set(largest)


def block_levels(rng, shape, split, least, top_value):
    factor_of = 1.0
    for axis_at, blocks in split:
        steps = jax.random.uniform(jax.random.fold_in(jax.random.fold_in(rng, 6), axis_at), (blocks,), jnp.float32, least / len(split), top_value / len(split))
        factor_of = factor_of * jnp.repeat(jnp.exp(steps), shape[axis_at] // blocks).reshape((-1,) + (1,) * (len(shape) - 1 - axis_at))
    return factor_of


def rank_bounds(number_of, skew):
    loads = [(1 << 20) // math.isqrt(rank ** skew) + 1 for rank in range(1, number_of + 1)]
    spread = 1 + sum(loads) // (1 << 30)
    return np.cumsum(np.array([max(1, weight // spread) for weight in loads]))


def ranked(own_key, extent, count, skew):
    listing = rank_bounds(count, skew)
    ticket = jax.random.randint(jax.random.fold_in(own_key, 1), extent, 0, int(listing[count - 1]))
    rank = jnp.searchsorted(jnp.asarray(listing, jnp.int32), ticket, side="right")
    return jax.random.permutation(jax.random.fold_in(own_key, 2), count)[rank].astype(jnp.int32)


def split_up(count, total, reach, lean):
    loads = [(1 << 20) // math.isqrt(rank ** lean) + 1 for rank in range(2, count + 1)]
    surplus, given = total - reach - (count - 1), [1] * (count - 1)
    while surplus > 0:
        movable = [i for i in range(count - 1) if given[i] < reach]
        whole, budget = sum([loads[i] for i in movable]), surplus
        for i in movable:
            more = min(reach - given[i], max(1, budget * loads[i] // whole), surplus)
            given[i] = given[i] + more
            surplus = surplus - more
    return np.array([reach] + given)


def uneven_parts(rng, amount, total, bound, lean):
    if amount == 2:
        one = jax.random.randint(rng, (), max(1, total - bound), min(bound, total - 1) + 1)
        return jnp.stack([one, total - one])
    lengths = jnp.asarray(split_up(amount, total, bound, lean), jnp.int32)
    couples = (amount - 1) // 2
    donor, taker = lengths[1:1 + 2 * couples:2], lengths[2:2 + 2 * couples:2]
    slack = jnp.minimum(donor - 1, bound - taker)
    passed = jax.random.randint(jax.random.fold_in(rng, 1), (couples,), 0, 1 << 20) % (slack + 1)
    lengths = lengths.at[1:1 + 2 * couples:2].set(donor - passed).at[2:2 + 2 * couples:2].set(taker + passed)
    return lengths[jax.random.permutation(jax.random.fold_in(rng, 2), amount)]


def noise(rng, extent, scale, most, cuts=(), kind=jnp.bfloat16):
    loudness = block_levels(rng, extent, cuts, -0.22, 0.18) if cuts else 1.0
    result = jax.random.normal(rng, extent, jnp.float32) * scale * loudness
    return jnp.minimum(jnp.maximum(result, -most), most).astype(kind)


def setup_inputs(seed: int = 0) -> dict:
    keys = jax.random.split(jax.random.key(seed), 21)
    return {
        "nodes": noise(keys[0], (NODES, D), 1.0, 6.0, ((0, 32),)),
        "edges": noise(keys[1], (SLOTS, D), 1.0, 6.0, ((0, 32),)),
        "send_nodes": set_ends(jax.random.randint(keys[2], (SLOTS,), 0, NODE_DEV), jax.random.fold_in(keys[2], 1), 0, NODE_DEV - 1).astype(jnp.int32),
        "block_tile": set_ends(ranked(keys[3], (NBLOCKS,), TILES_DEV, 2), jax.random.fold_in(keys[3], 3), 0, TILES_DEV - 1).astype(jnp.int32),
        "block_count": uneven_parts(keys[4], NBLOCKS, NBLOCKS * BLOCK * 6 // 10, BLOCK, 2).astype(jnp.int32),
        "slot_ids": set_ends(jax.random.randint(keys[5], (SLOTS,), 0, BLOCK), jax.random.fold_in(keys[5], 1), 0, BLOCK - 1).astype(jnp.int32),
        "edge_in_weight": noise(keys[6], (3 * D, D), (3 * D) ** -0.5, 0.4375),
        "edge_in_bias": noise(keys[7], (D,), 0.5, 3.0, (), jnp.float32),
        "edge_out_weight": noise(keys[8], (D, D), D ** -0.5, 0.75),
        "edge_out_bias": noise(keys[9], (D,), 0.5, 3.0, (), jnp.float32),
        "edge_gain": jnp.clip(jax.random.uniform(keys[10], (D,), jnp.float32, 0.5, 1.5), 0.5, 1.5),
        "edge_shift": noise(keys[11], (D,), 0.5, 3.0, (), jnp.float32),
        "node_in_weight": noise(keys[12], (2 * D, D), (2 * D) ** -0.5, 0.5),
        "node_in_bias": noise(keys[13], (D,), 0.5, 3.0, (), jnp.float32),
        "node_out_weight": noise(keys[14], (D, D), D ** -0.5, 0.75),
        "node_out_bias": noise(keys[15], (D,), 0.5, 3.0, (), jnp.float32),
        "node_gain": jnp.clip(jax.random.uniform(keys[16], (D,), jnp.float32, 0.5, 1.5), 0.5, 1.5),
        "node_shift": noise(keys[17], (D,), 0.5, 3.0, (), jnp.float32),
        "node_cot": noise(keys[18], (NODES, D), 1.0, 6.0, ((0, 32),)),
        "edge_cot": noise(keys[19], (SLOTS, D), 1.0, 6.0, ((0, 32),)),
    }


epsilon = 1e-05

@jax.custom_vjp
def low(v):
    return lax.optimization_barrier(v.astype(jnp.bfloat16)).astype(jnp.float32)

@jax.custom_vjp
def low_back(v):
    return v

def low_keep(v):
    return (low(v), None)

def low_pass(kept, grad):
    return (grad,)

def back_keep(v):
    return (v, None)

def back_low(kept, grad):
    return (low(grad),)
low.defvjp(low_keep, low_pass)
low_back.defvjp(back_keep, back_low)

def layer_norm(inputs, gain_vec, shift_vec):
    average = lax.optimization_barrier(jnp.mean(inputs, axis=-1, keepdims=True))
    centered = inputs - average
    variance = lax.optimization_barrier(jnp.mean(centered * centered, axis=-1, keepdims=True))
    return centered * lax.rsqrt(variance + epsilon) * gain_vec + shift_vec

def matmul(left_side, right_side):
    return jnp.dot(left_side, right_side, precision=lax.Precision.HIGHEST)

def routes(send_nodes, block_tile, block_count, slot_ids):
    tiles = block_tile.reshape(N_GRP, N_PEER, N_PEER, PEER_BLOCKS).transpose(0, 2, 1, 3)
    counts = block_count.reshape(N_GRP, N_PEER, N_PEER, PEER_BLOCKS).transpose(0, 2, 1, 3)
    slots = slot_ids.reshape(N_GRP, N_PEER, N_PEER, PEER_BLOCKS, BLOCK).transpose(0, 2, 1, 3, 4)
    group_ids = jnp.arange(N_GRP, dtype=jnp.int32).reshape(N_GRP, 1, 1, 1, 1)
    owner_ids = jnp.arange(N_PEER, dtype=jnp.int32).reshape(1, 1, N_PEER, 1, 1)
    places = jnp.arange(BLOCK, dtype=jnp.int32).reshape(1, 1, 1, 1, BLOCK)
    receiver = (group_ids * N_PEER + owner_ids) * NODE_DEV + tiles[..., None] * BLOCK + slots
    live = places < counts[..., None]
    devices = N_GRP * N_PEER
    sender = jnp.arange(devices, dtype=jnp.int32)[:, None] * NODE_DEV + send_nodes.reshape(devices, BLOCKS_DEV * BLOCK)
    return (sender, receiver.reshape(devices, BLOCKS_DEV * BLOCK).astype(jnp.int32), live.reshape(devices, BLOCKS_DEV * BLOCK))

def forward(nodes, edges, edge_in_weight, edge_in_bias, edge_out_weight, edge_out_bias, edge_gain, edge_shift, node_in_weight, node_in_bias, node_out_weight, node_out_bias, node_gain, node_shift, sender, receiver, live):
    devices = sender.shape[0]
    edge_blocks = edges.reshape(devices, -1, D)

    def edge_step(state_in, pieces):
        edge_piece, sender_piece, receiver_piece, live_piece = pieces
        sender_feats = nodes[sender_piece]
        receiver_feats = low_back(jnp.where(live_piece[:, None], nodes[receiver_piece], 0.0))
        edge_inputs = jnp.concatenate([sender_feats, receiver_feats, edge_piece], axis=1)
        first_pre = low_back(matmul(edge_inputs, edge_in_weight) + edge_in_bias)
        first_act = low(jax.nn.silu(first_pre))
        second_pre = low_back(matmul(first_act, edge_out_weight) + edge_out_bias)
        message = low(layer_norm(second_pre, edge_gain, edge_shift))
        edge_new = edge_piece + message
        message_sent = jnp.where(live_piece[:, None], low_back(message), 0.0)
        return (state_in, (edge_new, message_sent))
    unused, (edge_new, messages) = lax.scan(jax.checkpoint(edge_step), None, (edge_blocks, sender, receiver, live))
    aggregate = jax.ops.segment_sum(messages.reshape(-1, D), receiver.reshape(-1), num_segments=nodes.shape[0])
    node_inputs = jnp.concatenate([nodes, low(aggregate)], axis=1)
    third_pre = low_back(matmul(node_inputs, node_in_weight) + node_in_bias)
    third_act = low(jax.nn.silu(third_pre))
    fourth_pre = low_back(matmul(third_act, node_out_weight) + node_out_bias)
    node_new = nodes + layer_norm(fourth_pre, node_gain, node_shift)
    return (node_new, edge_new.reshape(edges.shape))

def reference(nodes, edges, send_nodes, block_tile, block_count, slot_ids, edge_in_weight, edge_in_bias, edge_out_weight, edge_out_bias, edge_gain, edge_shift, node_in_weight, node_in_bias, node_out_weight, node_out_bias, node_gain, node_shift, node_cot, edge_cot):
    sender, receiver, live = routes(send_nodes, block_tile, block_count, slot_ids)
    params = tuple((array_in.astype(jnp.float32) for array_in in (nodes, edges, edge_in_weight, edge_in_bias, edge_out_weight, edge_out_bias, edge_gain, edge_shift, node_in_weight, node_in_bias, node_out_weight, node_out_bias, node_gain, node_shift)))

    def layer(*arrays):
        return forward(*arrays, sender, receiver, live)
    outputs, pullback = jax.vjp(layer, *params)
    node_new, edge_new = outputs
    grads = pullback((node_cot.astype(jnp.float32), edge_cot.astype(jnp.float32)))
    return (node_new.astype(jnp.bfloat16), edge_new.astype(jnp.bfloat16), grads[0], grads[1], grads[2], grads[3], grads[4], grads[5], grads[6], grads[7], grads[8], grads[9], grads[10], grads[11], grads[12], grads[13])
```

```python
import functools

import jax
import jax.numpy as jnp
from jax import lax
from jax.experimental import pallas as pl
from jax.experimental.pallas import tpu as pltpu
from jax.sharding import PartitionSpec as P

epsilon = 1e-05
bf16 = jnp.bfloat16
f32 = jnp.float32
LANES = 128
WIDE = 256


def dot(left, right):
    return jnp.dot(left, right, preferred_element_type=f32)


def dot_nt(left, right):
    return lax.dot_general(left, right, (((1,), (1,)), ((), ())), preferred_element_type=f32)


def dot_exact(left, right):
    return jnp.dot(left, right, preferred_element_type=f32, precision=lax.Precision.HIGHEST)


def dot_nt_exact(left, right):
    return lax.dot_general(
        left,
        right,
        (((1,), (1,)), ((), ())),
        preferred_element_type=f32,
        precision=lax.Precision.HIGHEST,
    )


def params(limit=56):
    return pltpu.CompilerParams(vmem_limit_bytes=limit * 1024 * 1024)


def spread(column, width):
    return jnp.concatenate([column] * (width // LANES), axis=1)


def fold(values):
    total = values[:, :LANES]
    for start in range(LANES, values.shape[1], LANES):
        total = total + values[:, start : start + LANES]
    return total


def row_join(ref, first, count):
    return jnp.concatenate([ref[first + k : first + k + 1, :] for k in range(count)], axis=1)


def sigmoid(values):
    return 0.5 * jnp.tanh(0.5 * values) + 0.5


def onehot_rows(row, rows):
    width = row.shape[1]
    place = lax.broadcasted_iota(jnp.int32, (rows, width), 0)
    return jnp.where(place == row, 1.0, 0.0).astype(bf16)


def node_groups(node_ref):
    total = node_ref.shape[1]
    return jnp.concatenate(
        [node_ref[:, start : start + WIDE] for start in range(0, total, WIDE)], axis=0
    )


def sender_kernel(piece, node_ref, send_ref, edge_ref, weight_ref, vec_ref, pick_ref, base_ref):
    width = edge_ref.shape[1]
    feat = edge_ref.shape[0]
    groups = node_ref.shape[1] // WIDE
    table = node_groups(node_ref)
    bias = spread(vec_ref[0], piece)
    for start in range(0, width, piece):
        ids = row_join(send_ref, start // LANES, piece // LANES)
        onehot = onehot_rows(ids & (WIDE - 1), WIDE)
        group = lax.shift_right_logical(ids, 8)
        found = dot(table, onehot)
        rows = found[:feat]
        for g in range(1, groups):
            rows = jnp.where(
                jnp.broadcast_to(group == g, (feat, piece)), found[g * feat : (g + 1) * feat], rows
            )
        low = rows.astype(bf16)
        pick_ref[:, start : start + piece] = low
        both = jnp.concatenate([low, edge_ref[:, start : start + piece]], axis=0)
        base_ref[:, start : start + piece] = dot(weight_ref[...], both) + bias


def gather_blocks(meta_ref, first, code_ref, start, count, source_ref):
    feat = source_ref.shape[0]
    parts = []
    for k in range(count):
        block = start + k
        tile = meta_ref[first + block]
        code = code_ref[0, block : block + 1, :]
        index = jnp.broadcast_to(code & (LANES - 1), (feat, LANES))
        rows = source_ref[:, pl.ds(pl.multiple_of(tile * LANES, LANES), LANES)]
        taken = jnp.take_along_axis(rows, index, axis=1)
        parts.append(jnp.where(jnp.broadcast_to(code < LANES, (feat, LANES)), taken, 0.0))
    return jnp.concatenate(parts, axis=1)


def scatter_blocks(meta_ref, first, code_ref, start, count, values, total_ref):
    for k in range(count):
        block = start + k
        tile = meta_ref[first + block]
        onehot = onehot_rows(code_ref[0, block : block + 1, :], LANES)
        term = dot_nt(values[:, k * LANES : (k + 1) * LANES], onehot)
        where_to = pl.ds(pl.multiple_of(tile * LANES, LANES), LANES)
        total_ref[:, where_to] = total_ref[:, where_to] + term


def forward_kernel(peers, blocks, piece, meta_ref, code_ref, base_ref, edge_ref, in_ref, out_ref, vec_ref, *rest):
    shard_refs = rest[:peers]
    result_ref, act_ref, slope_ref, normed_ref, inv_ref, part_ref, proj_ref, total_ref = rest[peers:]
    step = pl.program_id(0)
    inner = pl.program_id(1)

    @pl.when(inner == 0)
    def _():
        for k in range(peers):

            @pl.when(step == k)
            def _():
                proj_ref[...] = dot(in_ref[...], shard_refs[k][...])

        total_ref[...] = jnp.zeros_like(total_ref)

    width = edge_ref.shape[1]
    first = 1 + (meta_ref[0] ^ step) * blocks + inner * (width // LANES)
    bias = spread(vec_ref[1], piece)
    gain = spread(vec_ref[2], piece)
    shift = spread(vec_ref[3], piece)
    per = piece // LANES
    for start in range(0, width, piece):
        lanes = slice(start, start + piece)
        pre = base_ref[:, lanes] + gather_blocks(meta_ref, first, code_ref, start // LANES, per, proj_ref)
        sig = sigmoid(pre)
        act = pre * sig
        slope_ref[:, lanes] = (sig + act * (1.0 - sig)).astype(bf16)
        act_low = act.astype(bf16)
        act_ref[:, lanes] = act_low
        second = dot(out_ref[...], act_low) + bias
        centered = second - jnp.mean(second, axis=0, keepdims=True)
        inv = lax.rsqrt(jnp.mean(centered * centered, axis=0, keepdims=True) + epsilon)
        normed = centered * inv
        normed_ref[:, lanes] = normed.astype(bf16)
        for k in range(per):
            inv_ref[start // LANES + k : start // LANES + k + 1, :] = inv[:, k * LANES : (k + 1) * LANES]
        message = (normed * gain + shift).astype(bf16)
        result_ref[:, lanes] = (edge_ref[:, lanes].astype(f32) + message.astype(f32)).astype(bf16)
        scatter_blocks(meta_ref, first, code_ref, start // LANES, per, message, total_ref)

    @pl.when(inner == pl.num_programs(1) - 1)
    def _():
        part_ref[0] = total_ref[...].astype(bf16)


def node_kernel(peers, node_ref, cot_ref, in_t_ref, in_ref, out_t_ref, out_ref, vec_ref, *rest):
    part_refs = rest[:peers]
    result_ref, base_ref, back_ref, pack_ref = rest[peers:]
    feat, total = node_ref.shape
    aggregate = part_refs[0][...].astype(f32)
    for k in range(1, peers):
        aggregate = aggregate + part_refs[k][...].astype(f32)
    node_inputs = jnp.concatenate([node_ref[...], aggregate.astype(bf16)], axis=0)
    pre = dot(in_t_ref[...], node_inputs) + spread(vec_ref[4], total)
    sig = sigmoid(pre)
    act = pre * sig
    slope = sig + act * (1.0 - sig)
    act_low = act.astype(bf16)
    second = dot(out_t_ref[...], act_low) + spread(vec_ref[5], total)
    centered = second - jnp.mean(second, axis=0, keepdims=True)
    inv = lax.rsqrt(jnp.mean(centered * centered, axis=0, keepdims=True) + epsilon)
    normed = centered * inv
    gain = spread(vec_ref[6], total)
    update = normed * gain + spread(vec_ref[7], total)
    result_ref[...] = (node_ref[...].astype(f32) + update).astype(bf16)
    upstream = cot_ref[...].astype(f32)
    scaled = upstream * gain
    inner = (
        scaled
        - jnp.mean(scaled, axis=0, keepdims=True)
        - normed * jnp.mean(scaled * normed, axis=0, keepdims=True)
    )
    grad = (inner * inv).astype(bf16)
    third = (dot(out_ref[...], grad) * slope).astype(bf16)
    input_grad = dot(in_ref[...], third)
    base_ref[...] = upstream + input_grad[:feat]
    back_ref[...] = input_grad[feat:].astype(bf16)
    pack_ref[...] = jnp.zeros_like(pack_ref)
    pack_ref[:feat, : 2 * feat] = dot_nt(third, node_inputs)
    pack_ref[:feat, 2 * feat : 3 * feat] = dot_nt(act_low, grad)
    ones = jnp.ones((8, LANES), f32)
    sums = (
        fold(third.astype(f32)),
        fold(grad.astype(f32)),
        fold(upstream * normed),
        fold(upstream),
    )
    for k in range(4):
        pack_ref[feat + k : feat + k + 1, :feat] = dot_nt_exact(ones, sums[k])[:1]


def backward_kernel(peers, blocks, piece, meta_ref, code_ref, cot_ref, normed_ref, act_ref, slope_ref, inv_ref, edge_ref, pick_ref, out_ref, in_ref, vec_ref, *rest):
    back_refs = rest[:peers]
    shard_refs = rest[peers : 2 * peers]
    grad_ref, first_ref, part_ref, pack_ref, pull_ref, total_ref, w1_ref, wr_ref, w2_ref, sum_ref = rest[2 * peers :]
    step = pl.program_id(0)
    inner = pl.program_id(1)
    feat, width = edge_ref.shape

    @pl.when((inner == 0) & (step == 0))
    def _():
        w1_ref[...] = jnp.zeros_like(w1_ref)
        wr_ref[...] = jnp.zeros_like(wr_ref)
        w2_ref[...] = jnp.zeros_like(w2_ref)
        sum_ref[...] = jnp.zeros_like(sum_ref)

    @pl.when(inner == 0)
    def _():
        for k in range(peers):

            @pl.when(step == k)
            def _():
                pull_ref[...] = back_refs[k][...].astype(f32)

        total_ref[...] = jnp.zeros_like(total_ref)

    first = 1 + (meta_ref[0] ^ step) * blocks + inner * (width // LANES)
    gain = spread(vec_ref[2], piece)
    per = piece // LANES
    for start in range(0, width, piece):
        lanes = slice(start, start + piece)
        cot = cot_ref[:, lanes].astype(f32)
        upstream = cot + gather_blocks(meta_ref, first, code_ref, start // LANES, per, pull_ref)
        normed = normed_ref[:, lanes].astype(f32)
        scaled = upstream * gain
        inner_grad = (
            scaled
            - jnp.mean(scaled, axis=0, keepdims=True)
            - normed * jnp.mean(scaled * normed, axis=0, keepdims=True)
        )
        inv = row_join(inv_ref, start // LANES, per)
        second = (inner_grad * inv).astype(bf16)
        sum_ref[2] += fold(upstream * normed)
        sum_ref[3] += fold(upstream)
        sum_ref[1] += fold(second.astype(f32))
        w2_ref[...] += dot_nt(act_ref[:, lanes], second)
        grad = (dot(out_ref[...], second) * slope_ref[:, lanes].astype(f32)).astype(bf16)
        first_ref[:, lanes] = grad
        sum_ref[0] += fold(grad.astype(f32))
        grad_ref[:, lanes] = cot + dot(in_ref[...], grad)
        both = jnp.concatenate([pick_ref[:, lanes], edge_ref[:, lanes]], axis=0)
        w1_ref[...] += dot_nt(grad, both)
        scatter_blocks(meta_ref, first, code_ref, start // LANES, per, grad, total_ref)

    @pl.when(inner == pl.num_programs(1) - 1)
    def _():
        low = total_ref[...].astype(bf16)
        part_ref[0] = low
        for k in range(peers):

            @pl.when(step == k)
            def _():
                wr_ref[...] += dot_nt(low, shard_refs[k][...])

    @pl.when((inner == pl.num_programs(1) - 1) & (step == pl.num_programs(0) - 1))
    def _():
        pack_ref[...] = jnp.zeros_like(pack_ref)
        pack_ref[:feat, :feat] = w1_ref[:, :feat]
        pack_ref[:feat, feat : 2 * feat] = wr_ref[...]
        pack_ref[:feat, 2 * feat : 3 * feat] = w1_ref[:, feat:]
        pack_ref[:feat, 3 * feat : 4 * feat] = w2_ref[...]
        ones = jnp.ones((8, LANES), f32)
        for k in range(4):
            pack_ref[feat + k : feat + k + 1, :feat] = dot_nt_exact(ones, sum_ref[k])[:1]


def sender_sum_kernel(grad_ref, send_ref, sum_ref, total_ref):
    feat, width = grad_ref.shape
    groups = sum_ref.shape[1] // WIDE

    @pl.when(pl.program_id(0) == 0)
    def _():
        total_ref[...] = jnp.zeros_like(total_ref)

    ids = row_join(send_ref, 0, width // LANES)
    onehot = onehot_rows(ids & (WIDE - 1), WIDE)
    group = jnp.broadcast_to(lax.shift_right_logical(ids, 8).astype(bf16), (feat, width))
    values = grad_ref[...]
    zero = jnp.zeros((), bf16)
    masked = jnp.concatenate(
        [jnp.where(group == jnp.asarray(g, bf16), values, zero) for g in range(groups)], axis=0
    )
    total_ref[...] += dot_nt(masked, onehot)

    @pl.when(pl.program_id(0) == pl.num_programs(0) - 1)
    def _():
        for g in range(groups):
            sum_ref[:, g * WIDE : (g + 1) * WIDE] = total_ref[g * feat : (g + 1) * feat, :]


def finish_kernel(peers, base_ref, sum_ref, weight_ref, node_pack_ref, edge_pack_ref, *rest):
    part_refs = rest[:peers]
    grad_ref, e1, b1, e2, b2, g1, s1, n1, c1, n2, c2, g2, s2 = rest[peers:]
    total = part_refs[0][...].astype(f32)
    for k in range(1, peers):
        total = total + part_refs[k][...].astype(f32)
    both = jnp.concatenate([sum_ref[...], total], axis=0)
    grad_ref[...] = base_ref[...] + dot_exact(weight_ref[...], both)
    feat = base_ref.shape[0]
    e1[...] = edge_pack_ref[:feat, : 3 * feat]
    e2[...] = edge_pack_ref[:feat, 3 * feat : 4 * feat]
    n1[...] = node_pack_ref[:feat, : 2 * feat]
    n2[...] = node_pack_ref[:feat, 2 * feat : 3 * feat]
    for k, ref in enumerate((b1, b2, g1, s1)):
        ref[...] = edge_pack_ref[feat + k : feat + k + 1, :feat]
    for k, ref in enumerate((c1, c2, g2, s2)):
        ref[...] = node_pack_ref[feat + k : feat + k + 1, :feat]


def struct(shape, dtype):
    return jax.ShapeDtypeStruct(shape, dtype)


def whole(shape):
    return pl.BlockSpec(shape, lambda *_: (0,) * len(shape))


def per_device(groups, peers, *arrays):
    (
        nodes, edges, send_nodes, block_tile, block_count, slot_ids,
        edge_in_weight, edge_in_bias, edge_out_weight, edge_out_bias, edge_gain, edge_shift,
        node_in_weight, node_in_bias, node_out_weight, node_out_bias, node_gain, node_shift,
        node_cot, edge_cot,
    ) = arrays
    feat = nodes.shape[1]
    node_total = nodes.shape[0]
    edge_total = edges.shape[0]
    block_total = block_tile.shape[0]
    blocks = block_total // peers
    per_peer = edge_total // peers
    rows = edge_total // LANES

    def swap(value, mask):
        if mask == 0:
            return value
        return lax.ppermute(value, "peer", [(i, i ^ mask) for i in range(peers)])

    def spread_out(value):
        return [swap(value, mask) for mask in range(peers)]

    def add_up(value):
        for axis, size in (("peer", peers), ("grp", groups)):
            mask = 1
            while mask < size:
                value = value + lax.ppermute(value, axis, [(i, i ^ mask) for i in range(size)])
                mask *= 2
        return value

    node_t = nodes.T
    edge_t = edges.T
    node_cot_t = node_cot.T
    edge_cot_t = edge_cot.T
    in_t = edge_in_weight.T
    send = send_nodes.reshape(rows, LANES)
    me = lax.axis_index("peer").astype(jnp.int32)

    shards = spread_out(node_t)

    live = jnp.arange(LANES, dtype=jnp.int32)[None, :] < block_count[:, None]
    code = slot_ids.reshape(block_total, LANES) + jnp.where(live, 0, LANES) + 2 * LANES * block_tile[:, None]
    code = lax.all_to_all(code, "peer", 0, 0, tiled=True)
    meta = jnp.concatenate([me[None], code[:, 0] // (2 * LANES)])
    code = (code & (2 * LANES - 1)).reshape(peers, blocks, LANES)

    vec = jnp.broadcast_to(
        jnp.stack([edge_in_bias, edge_out_bias, edge_gain, edge_shift, node_in_bias, node_out_bias, node_gain, node_shift])[:, :, None],
        (8, feat, LANES),
    )
    se_weight = jnp.concatenate([in_t[:, :feat], in_t[:, 2 * feat :]], axis=1)

    wide = 1024
    pick, base = pl.pallas_call(
        functools.partial(sender_kernel, 512),
        grid=(edge_total // wide,),
        in_specs=[
            whole((feat, node_total)),
            pl.BlockSpec((wide // LANES, LANES), lambda i: (i, 0)),
            pl.BlockSpec((feat, wide), lambda i: (0, i)),
            whole((feat, 2 * feat)),
            whole((8, feat, LANES)),
        ],
        out_specs=[
            pl.BlockSpec((feat, wide), lambda i: (0, i)),
            pl.BlockSpec((feat, wide), lambda i: (0, i)),
        ],
        out_shape=[struct((feat, edge_total), bf16), struct((feat, edge_total), f32)],
        compiler_params=params(),
        name="sender",
    )(node_t, send, edge_t, se_weight, vec)

    wide = min(1024, per_peer)
    chunks = per_peer // wide
    sub = wide // LANES

    def at(i, j, meta_ref):
        return (0, (meta_ref[0] ^ i) * chunks + j)

    def row_at(i, j, meta_ref):
        return ((meta_ref[0] ^ i) * chunks + j, 0)

    def code_at(i, j, meta_ref):
        return (meta_ref[0] ^ i, j, 0)

    slab = pl.BlockSpec((feat, wide), at)
    code_spec = pl.BlockSpec((1, sub, LANES), code_at)
    inv_spec = pl.BlockSpec((sub, LANES), row_at)
    shard_spec = whole((feat, node_total))
    part_spec = pl.BlockSpec((1, feat, node_total), lambda i, j, meta_ref: (i, 0, 0))
    edge_result, act, slope, normed, inv, part = pl.pallas_call(
        functools.partial(forward_kernel, peers, blocks, 512),
        grid_spec=pltpu.PrefetchScalarGridSpec(
            num_scalar_prefetch=1,
            grid=(peers, chunks),
            in_specs=[code_spec, slab, slab, whole((feat, feat)), whole((feat, feat)), whole((8, feat, LANES))]
            + [shard_spec] * peers,
            out_specs=[slab, slab, slab, slab, inv_spec, part_spec],
            scratch_shapes=[pltpu.VMEM((feat, node_total), f32), pltpu.VMEM((feat, node_total), f32)],
        ),
        out_shape=[
            struct((feat, edge_total), bf16),
            struct((feat, edge_total), bf16),
            struct((feat, edge_total), bf16),
            struct((feat, edge_total), bf16),
            struct((rows, LANES), f32),
            struct((peers, feat, node_total), bf16),
        ],
        compiler_params=params(),
        name="forward",
    )(meta, code, base, edge_t, in_t[:, feat : 2 * feat], edge_out_weight.T, vec, *shards)

    parts = [swap(part[mask], mask) for mask in range(peers)]
    node_result, node_base, back, node_pack = pl.pallas_call(
        functools.partial(node_kernel, peers),
        out_shape=[
            struct((feat, node_total), bf16),
            struct((feat, node_total), f32),
            struct((feat, node_total), bf16),
            struct((feat + 8, 4 * feat), f32),
        ],
        compiler_params=params(),
        name="node",
    )(node_t, node_cot_t, node_in_weight.T, node_in_weight, node_out_weight.T, node_out_weight, vec, *parts)

    backs = spread_out(back)
    node_pack = add_up(node_pack)

    edge_grad, first_grad, part, edge_pack = pl.pallas_call(
        functools.partial(backward_kernel, peers, blocks, 512),
        grid_spec=pltpu.PrefetchScalarGridSpec(
            num_scalar_prefetch=1,
            grid=(peers, chunks),
            in_specs=[code_spec, slab, slab, slab, slab, inv_spec, slab, slab, whole((feat, feat)), whole((feat, feat)), whole((8, feat, LANES))]
            + [shard_spec] * (2 * peers),
            out_specs=[slab, slab, part_spec, whole((feat + 8, 4 * feat))],
            scratch_shapes=[
                pltpu.VMEM((feat, node_total), f32),
                pltpu.VMEM((feat, node_total), f32),
                pltpu.VMEM((feat, 2 * feat), f32),
                pltpu.VMEM((feat, feat), f32),
                pltpu.VMEM((feat, feat), f32),
                pltpu.VMEM((4, feat, LANES), f32),
            ],
        ),
        out_shape=[
            struct((feat, edge_total), f32),
            struct((feat, edge_total), bf16),
            struct((peers, feat, node_total), bf16),
            struct((feat + 8, 4 * feat), f32),
        ],
        compiler_params=params(),
        name="backward",
    )(meta, code, edge_cot_t, normed, act, slope, inv, edge_t, pick, edge_out_weight, edge_in_weight[2 * feat :], vec, *backs, *shards)

    parts = [swap(part[mask], mask) for mask in range(peers)]
    edge_pack = add_up(edge_pack)

    wide = 2048
    send_sum = pl.pallas_call(
        sender_sum_kernel,
        grid=(edge_total // wide,),
        in_specs=[
            pl.BlockSpec((feat, wide), lambda i: (0, i)),
            pl.BlockSpec((wide // LANES, LANES), lambda i: (i, 0)),
        ],
        out_specs=whole((feat, node_total)),
        out_shape=struct((feat, node_total), f32),
        scratch_shapes=[pltpu.VMEM((node_total // WIDE * feat, WIDE), f32)],
        compiler_params=params(),
        name="sender_sum",
    )(first_grad, send)

    vec_out = struct((1, feat), f32)
    sr_weight = jnp.concatenate([edge_in_weight[:feat], edge_in_weight[feat : 2 * feat]], axis=1).astype(f32)
    node_grad, e1, b1, e2, b2, g1, s1, n1, c1, n2, c2, g2, s2 = pl.pallas_call(
        functools.partial(finish_kernel, peers),
        out_shape=[
            struct((feat, node_total), f32),
            struct((feat, 3 * feat), f32), vec_out, struct((feat, feat), f32), vec_out, vec_out, vec_out,
            struct((feat, 2 * feat), f32), vec_out, struct((feat, feat), f32), vec_out, vec_out, vec_out,
        ],
        compiler_params=params(),
        name="finish",
    )(node_base, send_sum, sr_weight, node_pack, edge_pack, *parts)

    def flat(row):
        return row.reshape(feat)

    return (
        node_result.T, edge_result.T, node_grad.T, edge_grad.T,
        e1.T, flat(b1), e2, flat(b2), flat(g1), flat(s1),
        n1.T, flat(c1), n2, flat(c2), flat(g2), flat(s2),
    )


def solution(mesh):
    split = P(("grp", "peer"), None)
    line = P(("grp", "peer"))
    one = P()
    return jax.shard_map(
        functools.partial(per_device, mesh.shape["grp"], mesh.shape["peer"]),
        mesh=mesh,
        in_specs=(split, split, line, line, line, line) + (one,) * 12 + (split, split),
        out_specs=(split, split, split, split) + (one,) * 12,
        check_vma=False,
    )
```

```python
import functools

import jax
import jax.numpy as jnp
from jax import lax
from jax.experimental import pallas as pl
from jax.experimental.pallas import tpu as pltpu
from jax.sharding import PartitionSpec as P

epsilon = 1e-05
bf16 = jnp.bfloat16
f32 = jnp.float32
LANES = 128
WIDE = 256


def dot(left, right):
    return jnp.dot(left, right, preferred_element_type=f32)


def dot_nt(left, right):
    return lax.dot_general(left, right, (((1,), (1,)), ((), ())), preferred_element_type=f32)


def dot_exact(left, right):
    return jnp.dot(left, right, preferred_element_type=f32, precision=lax.Precision.HIGHEST)


def dot_nt_exact(left, right):
    return lax.dot_general(
        left,
        right,
        (((1,), (1,)), ((), ())),
        preferred_element_type=f32,
        precision=lax.Precision.HIGHEST,
    )


def params(limit=56):
    return pltpu.CompilerParams(vmem_limit_bytes=limit * 1024 * 1024)


def spread(column, width):
    return jnp.concatenate([column] * (width // LANES), axis=1)


def fold(values):
    total = values[:, :LANES]
    for start in range(LANES, values.shape[1], LANES):
        total = total + values[:, start : start + LANES]
    return total


def row_join(ref, first, count):
    return jnp.concatenate([ref[first + k : first + k + 1, :] for k in range(count)], axis=1)


def sigmoid(values):
    return 0.5 * jnp.tanh(0.5 * values) + 0.5


def onehot_rows(row, rows):
    width = row.shape[1]
    place = lax.broadcasted_iota(jnp.int32, (rows, width), 0)
    return jnp.where(place == row, 1.0, 0.0).astype(bf16)


def onehot_low(row, place):
    spots = jnp.broadcast_to(row.astype(bf16), place.shape)
    return jnp.where(place == spots, jnp.ones((), bf16), jnp.zeros((), bf16))


def place_low():
    return lax.broadcasted_iota(jnp.int32, (LANES, LANES), 0).astype(bf16)


def node_groups(node_ref):
    total = node_ref.shape[1]
    return jnp.concatenate(
        [node_ref[:, start : start + WIDE] for start in range(0, total, WIDE)], axis=0
    )


def sender_kernel(piece, me_ref, node_ref, send_ref, edge_ref, weight_ref, vec_ref, pick_ref, base_ref):
    width = edge_ref.shape[1]
    feat = edge_ref.shape[0]
    groups = node_ref.shape[1] // WIDE
    table = node_groups(node_ref)
    bias = spread(vec_ref[0], piece)
    for start in range(0, width, piece):
        ids = row_join(send_ref, start // LANES, piece // LANES)
        onehot = onehot_rows(ids & (WIDE - 1), WIDE)
        group = lax.shift_right_logical(ids, 8)
        found = dot(table, onehot)
        rows = found[:feat]
        for g in range(1, groups):
            rows = jnp.where(
                jnp.broadcast_to(group == g, (feat, piece)), found[g * feat : (g + 1) * feat], rows
            )
        low = rows.astype(bf16)
        pick_ref[:, start : start + piece] = low
        both = jnp.concatenate([low, edge_ref[:, start : start + piece]], axis=0)
        base_ref[:, start : start + piece] = dot(weight_ref[...], both) + bias


def gather_blocks(meta_ref, first, code_ref, start, count, source_ref):
    feat = source_ref.shape[0]
    parts = []
    for k in range(count):
        tile = meta_ref[first + start + k]
        code = code_ref[0, start + k : start + k + 1, :]
        index = jnp.broadcast_to(code & (LANES - 1), (feat, LANES))
        rows = source_ref[:, pl.ds(pl.multiple_of(tile * LANES, LANES), LANES)]
        taken = jnp.take_along_axis(rows, index, axis=1)
        parts.append(jnp.where(jnp.broadcast_to(code < LANES, (feat, LANES)), taken, 0.0))
    return jnp.concatenate(parts, axis=1)


def scatter_blocks(meta_ref, first, code_ref, start, count, values, total_ref, place):
    for k in range(count):
        tile = meta_ref[first + start + k]
        onehot = onehot_low(code_ref[0, start + k : start + k + 1, :], place)
        term = dot_nt(values[:, k * LANES : (k + 1) * LANES], onehot)
        where_to = pl.ds(pl.multiple_of(tile * LANES, LANES), LANES)
        total_ref[:, where_to] = total_ref[:, where_to] + term


def forward_kernel(masks, blocks, piece, extra, meta_ref, code_ref, base_ref, edge_ref, in_ref, out_ref, vec_ref, *rest):
    count = len(masks)
    shard_refs = rest[:count]
    result_ref, act_ref, slope_ref, normed_ref, inv_ref, part_ref, proj_ref, total_ref = rest[count + extra :]
    step = pl.program_id(0)
    for k in range(count):

        @pl.when(step == k)
        def _():
            proj_ref[...] = dot(in_ref[...], shard_refs[k][...])

    total_ref[...] = jnp.zeros_like(total_ref)
    width = edge_ref.shape[1]
    first = 1 + owner(masks, step, meta_ref) * blocks
    per = piece // LANES
    place = place_low()
    for start in range(0, width, piece):
        lanes = slice(start, start + piece)
        block = start // LANES
        half = base_ref[:, lanes] + gather_blocks(meta_ref, first, code_ref, block, per, proj_ref)
        up = jnp.tanh(half) + 1.0
        act = half * up
        slope_ref[:, lanes] = (up + act * (2.0 - up)).astype(bf16)
        act_low = act.astype(bf16)
        act_ref[:, lanes] = act_low
        second = dot(out_ref[...], act_low) + spread(vec_ref[1], piece)
        centered = second - jnp.mean(second, axis=0, keepdims=True)
        inv = lax.rsqrt(jnp.mean(centered * centered, axis=0, keepdims=True) + epsilon)
        normed = centered * inv
        normed_ref[:, lanes] = normed.astype(bf16)
        for k in range(per):
            inv_ref[block + k : block + k + 1, :] = inv[:, k * LANES : (k + 1) * LANES]
        message = (normed * spread(vec_ref[2], piece) + spread(vec_ref[3], piece)).astype(bf16)
        result_ref[:, lanes] = edge_ref[:, lanes] + message
        scatter_blocks(meta_ref, first, code_ref, block, per, message, total_ref, place)
    part_ref[0] = total_ref[...].astype(bf16)


def node_kernel(peers, node_ref, cot_ref, in_t_ref, in_ref, out_t_ref, out_ref, vec_ref, *rest):
    part_refs = rest[:peers]
    result_ref, base_ref, back_ref, pack_ref = rest[peers:]
    feat, total = node_ref.shape
    aggregate = part_refs[0][...].astype(f32)
    for k in range(1, peers):
        aggregate = aggregate + part_refs[k][...].astype(f32)
    node_inputs = jnp.concatenate([node_ref[...], aggregate.astype(bf16)], axis=0)
    pre = dot(in_t_ref[...], node_inputs) + spread(vec_ref[4], total)
    sig = sigmoid(pre)
    act = pre * sig
    slope = sig + act * (1.0 - sig)
    act_low = act.astype(bf16)
    second = dot(out_t_ref[...], act_low) + spread(vec_ref[5], total)
    centered = second - jnp.mean(second, axis=0, keepdims=True)
    inv = lax.rsqrt(jnp.mean(centered * centered, axis=0, keepdims=True) + epsilon)
    normed = centered * inv
    gain = spread(vec_ref[6], total)
    update = normed * gain + spread(vec_ref[7], total)
    result_ref[...] = (node_ref[...].astype(f32) + update).astype(bf16)
    upstream = cot_ref[...].astype(f32)
    scaled = upstream * gain
    inner = (
        scaled
        - jnp.mean(scaled, axis=0, keepdims=True)
        - normed * jnp.mean(scaled * normed, axis=0, keepdims=True)
    )
    grad = (inner * inv).astype(bf16)
    third = (dot(out_ref[...], grad) * slope).astype(bf16)
    input_grad = dot(in_ref[...], third)
    base_ref[...] = upstream + input_grad[:feat]
    back_ref[...] = input_grad[feat:].astype(bf16)
    pack_ref[...] = jnp.zeros_like(pack_ref)
    pack_ref[:feat, : 2 * feat] = dot_nt(third, node_inputs)
    pack_ref[:feat, 2 * feat : 3 * feat] = dot_nt(act_low, grad)
    ones = jnp.ones((8, LANES), f32)
    sums = (
        fold(third.astype(f32)),
        fold(grad.astype(f32)),
        fold(upstream * normed),
        fold(upstream),
    )
    for k in range(4):
        pack_ref[feat + k : feat + k + 1, :feat] = dot_nt_exact(ones, sums[k])[:1]


def backward_kernel(masks, blocks, piece, extra, meta_ref, code_ref, cot_ref, normed_ref, act_ref, slope_ref, inv_ref, edge_ref, pick_ref, out_ref, in_ref, vec_ref, *rest):
    count = len(masks)
    back_refs = rest[:count]
    shard_refs = rest[count : 2 * count]
    prior_refs = rest[2 * count : 2 * count + extra]
    grad_ref, first_ref, part_ref, pack_ref, pull_ref, total_ref, w1_ref, wr_ref, w2_ref, sum_ref = rest[2 * count + extra :]
    step = pl.program_id(0)
    feat, width = edge_ref.shape

    @pl.when(step == 0)
    def _():
        w1_ref[...] = jnp.zeros_like(w1_ref)
        wr_ref[...] = jnp.zeros_like(wr_ref)
        w2_ref[...] = jnp.zeros_like(w2_ref)
        sum_ref[...] = jnp.zeros_like(sum_ref)

    for k in range(count):

        @pl.when(step == k)
        def _():
            pull_ref[...] = back_refs[k][...].astype(f32)

    total_ref[...] = jnp.zeros_like(total_ref)
    first = 1 + owner(masks, step, meta_ref) * blocks
    per = piece // LANES
    place = place_low()
    for start in range(0, width, piece):
        lanes = slice(start, start + piece)
        block = start // LANES
        cot = cot_ref[:, lanes].astype(f32)
        upstream = cot + gather_blocks(meta_ref, first, code_ref, block, per, pull_ref)
        normed = normed_ref[:, lanes].astype(f32)
        scaled = upstream * spread(vec_ref[2], piece)
        inner_grad = (
            scaled
            - jnp.mean(scaled, axis=0, keepdims=True)
            - normed * jnp.mean(scaled * normed, axis=0, keepdims=True)
        )
        second = (inner_grad * row_join(inv_ref, block, per)).astype(bf16)
        sum_ref[2] += fold(upstream * normed)
        sum_ref[3] += fold(upstream)
        sum_ref[1] += fold(second.astype(f32))
        w2_ref[...] += dot_nt(act_ref[:, lanes], second)
        grad = (dot(out_ref[...], second) * slope_ref[:, lanes].astype(f32)).astype(bf16)
        first_ref[:, lanes] = grad
        sum_ref[0] += fold(grad.astype(f32))
        grad_ref[:, lanes] = cot + dot(in_ref[...], grad)
        both = jnp.concatenate([pick_ref[:, lanes], edge_ref[:, lanes]], axis=0)
        w1_ref[...] += dot_nt(grad, both)
        scatter_blocks(meta_ref, first, code_ref, block, per, grad, total_ref, place)
    low = total_ref[...].astype(bf16)
    part_ref[0] = low
    for k in range(count):

        @pl.when(step == k)
        def _():
            wr_ref[...] += dot_nt(low, shard_refs[k][...])

    @pl.when(step == pl.num_programs(0) - 1)
    def _():
        pack_ref[...] = jnp.zeros_like(pack_ref)
        pack_ref[:feat, :feat] = w1_ref[:, :feat]
        pack_ref[:feat, feat : 2 * feat] = wr_ref[...]
        pack_ref[:feat, 2 * feat : 3 * feat] = w1_ref[:, feat:]
        pack_ref[:feat, 3 * feat : 4 * feat] = w2_ref[...]
        ones = jnp.ones((8, LANES), f32)
        for k in range(4):
            pack_ref[feat + k : feat + k + 1, :feat] = dot_nt_exact(ones, sum_ref[k])[:1]
        if extra:
            pack_ref[...] += prior_refs[1][...]


def sender_sum_kernel(me_ref, grad_ref, send_ref, sum_ref, total_ref):
    feat, width = grad_ref.shape
    groups = sum_ref.shape[1] // WIDE

    @pl.when(pl.program_id(0) == 0)
    def _():
        total_ref[...] = jnp.zeros_like(total_ref)

    piece = min(2048, width)
    for start in range(0, width, piece):
        ids = row_join(send_ref, start // LANES, piece // LANES)
        onehot = onehot_rows(ids & (WIDE - 1), WIDE)
        group = jnp.broadcast_to(lax.shift_right_logical(ids, 8).astype(bf16), (feat, piece))
        values = grad_ref[:, start : start + piece]
        zero = jnp.zeros((), bf16)
        masked = jnp.concatenate(
            [jnp.where(group == jnp.asarray(g, bf16), values, zero) for g in range(groups)], axis=0
        )
        total_ref[...] += dot_nt(masked, onehot)

    @pl.when(pl.program_id(0) == pl.num_programs(0) - 1)
    def _():
        for g in range(groups):
            sum_ref[:, g * WIDE : (g + 1) * WIDE] = total_ref[g * feat : (g + 1) * feat, :]


def finish_kernel(sums, peers, base_ref, weight_ref, node_pack_ref, edge_pack_ref, *rest):
    sum_refs = rest[:sums]
    part_refs = rest[sums : sums + peers]
    grad_ref, e1, b1, e2, b2, g1, s1, n1, c1, n2, c2, g2, s2 = rest[sums + peers :]
    sent = sum_refs[0][...]
    for k in range(1, sums):
        sent = sent + sum_refs[k][...]
    total = part_refs[0][...].astype(f32)
    for k in range(1, peers):
        total = total + part_refs[k][...].astype(f32)
    both = jnp.concatenate([sent, total], axis=0)
    grad_ref[...] = base_ref[...] + dot_exact(weight_ref[...], both)
    feat = base_ref.shape[0]
    e1[...] = edge_pack_ref[:feat, : 3 * feat]
    e2[...] = edge_pack_ref[:feat, 3 * feat : 4 * feat]
    n1[...] = node_pack_ref[:feat, : 2 * feat]
    n2[...] = node_pack_ref[:feat, 2 * feat : 3 * feat]
    for k, ref in enumerate((b1, b2, g1, s1)):
        ref[...] = edge_pack_ref[feat + k : feat + k + 1, :feat]
    for k, ref in enumerate((c1, c2, g2, s2)):
        ref[...] = node_pack_ref[feat + k : feat + k + 1, :feat]


def owner(masks, step, meta_ref):
    stride = masks[1] - masks[0] if len(masks) > 1 else 0
    return meta_ref[0] ^ (masks[0] + stride * step)


def struct(shape, dtype):
    return jax.ShapeDtypeStruct(shape, dtype)


def whole(shape):
    return pl.BlockSpec(shape, lambda *_: (0,) * len(shape))


def per_device(groups, peers, *arrays):
    (
        nodes, edges, send_nodes, block_tile, block_count, slot_ids,
        edge_in_weight, edge_in_bias, edge_out_weight, edge_out_bias, edge_gain, edge_shift,
        node_in_weight, node_in_bias, node_out_weight, node_out_bias, node_gain, node_shift,
        node_cot, edge_cot,
    ) = arrays
    feat = nodes.shape[1]
    node_total = nodes.shape[0]
    edge_total = edges.shape[0]
    block_total = block_tile.shape[0]
    blocks = block_total // peers
    per_peer = edge_total // peers
    rows = edge_total // LANES

    def swap(value, mask):
        if mask == 0:
            return value
        return lax.ppermute(value, "peer", [(i, i ^ mask) for i in range(peers)])

    near = [m for m in range(0, peers, 2)]
    routed = [m for m in (4, 6, 2) if m < peers] + [m for m in range(8, peers, 2)]

    def gather_all(value):
        found = {0: value, 1: swap(value, 1)}
        for m in routed:
            found[m] = swap(value, m)
        for m in routed:
            found[m | 1] = swap(found[m], 1)
        return found

    def sum_out(parts):
        got = {m: swap(parts[m | 1], 1) for m in routed + [0]}
        sums = [parts[0], got[0]]
        for m in routed:
            both = (parts[m].astype(f32) + got[m].astype(f32)).astype(bf16)
            sums.append(swap(both, m))
        return sums

    def add_up(value):
        for axis, size in (("grp", groups), ("peer", peers)):
            mask = 1
            while mask < size:
                value = value + lax.ppermute(value, axis, [(i, i ^ mask) for i in range(size)])
                mask *= 2
        return value

    teams = [tuple(range(0, peers, 2)), tuple(range(1, peers, 2))]

    node_t = nodes.T
    edge_t = edges.T
    node_cot_t = node_cot.T
    edge_cot_t = edge_cot.T
    in_t = edge_in_weight.T
    send = send_nodes.reshape(rows, LANES)
    me = lax.axis_index("peer").astype(jnp.int32)[None]

    shards = gather_all(node_t)

    live = jnp.arange(LANES, dtype=jnp.int32)[None, :] < block_count[:, None]
    code = slot_ids.reshape(block_total, LANES) + jnp.where(live, 0, LANES) + 2 * LANES * block_tile[:, None]
    code = lax.all_to_all(code, "peer", 0, 0, tiled=True)
    meta = jnp.concatenate([me, code[:, 0] // (2 * LANES)])
    code = (code & (2 * LANES - 1)).reshape(peers, blocks, LANES)

    vec = jnp.broadcast_to(
        jnp.stack([0.5 * edge_in_bias, edge_out_bias, edge_gain, edge_shift, node_in_bias, node_out_bias, node_gain, node_shift])[:, :, None],
        (8, feat, LANES),
    )
    half = jnp.asarray(0.5, bf16)
    se_weight = jnp.concatenate([in_t[:, :feat], in_t[:, 2 * feat :]], axis=1) * half
    re_weight = in_t[:, feat : 2 * feat] * half
    back_weight = edge_out_weight * half

    wide = per_peer
    sub = wide // LANES

    def slab_of(masks):
        return pl.BlockSpec((feat, wide), lambda i, ref: (0, owner(masks, i, ref)))

    def rows_of(masks):
        return pl.BlockSpec((sub, LANES), lambda i, ref: (owner(masks, i, ref), 0))

    def code_of(masks):
        return pl.BlockSpec((1, sub, LANES), lambda i, ref: (owner(masks, i, ref), 0, 0))

    own_slab = pl.BlockSpec((feat, wide), lambda i, ref: (0, i))
    own_rows = pl.BlockSpec((sub, LANES), lambda i, ref: (i, 0))
    part_spec = pl.BlockSpec((1, feat, node_total), lambda i, ref: (i, 0, 0))
    shard_spec = whole((feat, node_total))
    keep_spec = pl.BlockSpec(memory_space=pl.ANY)

    picks, bases = [], []
    for masks in teams:
        count = len(masks)
        pick, base = pl.pallas_call(
            functools.partial(sender_kernel, 512),
            grid_spec=pltpu.PrefetchScalarGridSpec(
                num_scalar_prefetch=1,
                grid=(count,),
                in_specs=[shard_spec, rows_of(masks), slab_of(masks), whole((feat, 2 * feat)), whole((8, feat, LANES))],
                out_specs=[own_slab, own_slab],
            ),
            out_shape=[struct((feat, count * wide), bf16), struct((feat, count * wide), f32)],
            compiler_params=params(),
            name="sender",
        )(me, node_t, send, edge_t, se_weight, vec)
        picks.append(pick)
        bases.append(base)

    saved = []
    parts = {}
    result = None
    for t, masks in enumerate(teams):
        count = len(masks)
        extra = 0 if result is None else 1
        result, act, slope, normed, inv, part = pl.pallas_call(
            functools.partial(forward_kernel, masks, blocks, 1024, extra),
            grid_spec=pltpu.PrefetchScalarGridSpec(
                num_scalar_prefetch=1,
                grid=(count,),
                in_specs=[code_of(masks), own_slab, slab_of(masks), whole((feat, feat)), whole((feat, feat)), whole((8, feat, LANES))]
                + [shard_spec] * count
                + [keep_spec] * extra,
                out_specs=[slab_of(masks), own_slab, own_slab, own_slab, own_rows, part_spec],
                scratch_shapes=[pltpu.VMEM((feat, node_total), f32), pltpu.VMEM((feat, node_total), f32)],
            ),
            out_shape=[
                struct((feat, edge_total), bf16),
                struct((feat, count * wide), bf16),
                struct((feat, count * wide), bf16),
                struct((feat, count * wide), bf16),
                struct((count * sub, LANES), f32),
                struct((count, feat, node_total), bf16),
            ],
            input_output_aliases={7 + count: 0} if extra else {},
            compiler_params=params(),
            name="forward",
        )(meta, code, bases[t], edge_t, re_weight, edge_out_weight.T, vec, *[shards[m] for m in masks], *([result] * extra))
        saved.append((normed, act, slope, inv))
        for k, m in enumerate(masks):
            parts[m] = part[k]
    edge_result = result

    sums = sum_out(parts)
    node_result, node_base, back, node_pack = pl.pallas_call(
        functools.partial(node_kernel, len(sums)),
        out_shape=[
            struct((feat, node_total), bf16),
            struct((feat, node_total), f32),
            struct((feat, node_total), bf16),
            struct((feat + 8, 4 * feat), f32),
        ],
        compiler_params=params(),
        name="node",
    )(node_t, node_cot_t, node_in_weight.T, node_in_weight, node_out_weight.T, node_out_weight, vec, *sums)

    backs = gather_all(back)
    node_pack = add_up(node_pack)

    parts = {}
    firsts = []
    edge_grad = edge_pack = None
    for t, masks in enumerate(teams):
        count = len(masks)
        prior = [] if edge_grad is None else [edge_grad, edge_pack]
        extra = len(prior)
        normed, act, slope, inv = saved[t]
        edge_grad, first_grad, part, edge_pack = pl.pallas_call(
            functools.partial(backward_kernel, masks, blocks, 1024, extra),
            grid_spec=pltpu.PrefetchScalarGridSpec(
                num_scalar_prefetch=1,
                grid=(count,),
                in_specs=[code_of(masks), slab_of(masks), own_slab, own_slab, own_slab, own_rows, slab_of(masks), own_slab, whole((feat, feat)), whole((feat, feat)), whole((8, feat, LANES))]
                + [shard_spec] * (2 * count)
                + ([keep_spec, whole((feat + 8, 4 * feat))] if extra else []),
                out_specs=[slab_of(masks), own_slab, part_spec, whole((feat + 8, 4 * feat))],
                scratch_shapes=[
                    pltpu.VMEM((feat, node_total), f32),
                    pltpu.VMEM((feat, node_total), f32),
                    pltpu.VMEM((feat, 2 * feat), f32),
                    pltpu.VMEM((feat, feat), f32),
                    pltpu.VMEM((feat, feat), f32),
                    pltpu.VMEM((4, feat, LANES), f32),
                ],
            ),
            out_shape=[
                struct((feat, edge_total), f32),
                struct((feat, count * wide), bf16),
                struct((count, feat, node_total), bf16),
                struct((feat + 8, 4 * feat), f32),
            ],
            input_output_aliases={12 + 2 * count: 0} if extra else {},
            compiler_params=params(),
            name="backward",
        )(
            meta, code, edge_cot_t, normed, act, slope, inv, edge_t, picks[t], back_weight, edge_in_weight[2 * feat :], vec,
            *[backs[m] for m in masks], *[shards[m] for m in masks], *prior,
        )
        firsts.append(first_grad)
        for k, m in enumerate(masks):
            parts[m] = part[k]

    sums = sum_out(parts)
    edge_pack = add_up(edge_pack)

    sent = []
    for t, masks in enumerate(teams):
        sent.append(
            pl.pallas_call(
                sender_sum_kernel,
                grid_spec=pltpu.PrefetchScalarGridSpec(
                    num_scalar_prefetch=1,
                    grid=(len(masks),),
                    in_specs=[own_slab, rows_of(masks)],
                    out_specs=shard_spec,
                    scratch_shapes=[pltpu.VMEM((node_total // WIDE * feat, WIDE), f32)],
                ),
                out_shape=struct((feat, node_total), f32),
                compiler_params=params(),
                name="sender_sum",
            )(me, firsts[t], send)
        )

    vec_out = struct((1, feat), f32)
    sr_weight = jnp.concatenate([edge_in_weight[:feat], edge_in_weight[feat : 2 * feat]], axis=1).astype(f32)
    node_grad, e1, b1, e2, b2, g1, s1, n1, c1, n2, c2, g2, s2 = pl.pallas_call(
        functools.partial(finish_kernel, len(sent), len(sums)),
        out_shape=[
            struct((feat, node_total), f32),
            struct((feat, 3 * feat), f32), vec_out, struct((feat, feat), f32), vec_out, vec_out, vec_out,
            struct((feat, 2 * feat), f32), vec_out, struct((feat, feat), f32), vec_out, vec_out, vec_out,
        ],
        compiler_params=params(),
        name="finish",
    )(node_base, sr_weight, node_pack, edge_pack, *sent, *sums)

    def flat(row):
        return row.reshape(feat)

    return (
        node_result.T, edge_result.T, node_grad.T, edge_grad.T,
        e1.T, flat(b1), e2, flat(b2), flat(g1), flat(s1),
        n1.T, flat(c1), n2, flat(c2), flat(g2), flat(s2),
    )


def solution(mesh):
    split = P(("grp", "peer"), None)
    line = P(("grp", "peer"))
    one = P()
    return jax.shard_map(
        functools.partial(per_device, mesh.shape["grp"], mesh.shape["peer"]),
        mesh=mesh,
        in_specs=(split, split, line, line, line, line) + (one,) * 12 + (split, split),
        out_specs=(split, split, split, split) + (one,) * 12,
        check_vma=False,
    )
```

```python
import functools

import jax
import jax.numpy as jnp
from jax import lax
from jax.experimental import pallas as pl
from jax.experimental.pallas import tpu as pltpu
from jax.sharding import PartitionSpec as P

epsilon = 1e-05
bf16 = jnp.bfloat16
f32 = jnp.float32
LANES = 128
WIDE = 256


def dot(left, right):
    return jnp.dot(left, right, preferred_element_type=f32)


def dot_nt(left, right):
    return lax.dot_general(left, right, (((1,), (1,)), ((), ())), preferred_element_type=f32)


def dot_exact(left, right):
    return jnp.dot(left, right, preferred_element_type=f32, precision=lax.Precision.HIGHEST)


def dot_nt_exact(left, right):
    return lax.dot_general(
        left,
        right,
        (((1,), (1,)), ((), ())),
        preferred_element_type=f32,
        precision=lax.Precision.HIGHEST,
    )


def params(limit=48):
    return pltpu.CompilerParams(vmem_limit_bytes=limit * 1024 * 1024)


def spread(column, width):
    return jnp.concatenate([column] * (width // LANES), axis=1)


def fold(values):
    total = values[:, :LANES]
    for start in range(LANES, values.shape[1], LANES):
        total = total + values[:, start : start + LANES]
    return total


def row_join(ref, first, count):
    return jnp.concatenate([ref[first + k : first + k + 1, :] for k in range(count)], axis=1)


def sigmoid(values):
    return 0.5 * jnp.tanh(0.5 * values) + 0.5


def onehot_rows(row, rows):
    width = row.shape[1]
    place = lax.broadcasted_iota(jnp.int32, (rows, width), 0)
    return jnp.where(place == row, 1.0, 0.0).astype(bf16)


def onehot_low(row, place):
    spots = jnp.broadcast_to(row.astype(bf16), place.shape)
    return jnp.where(place == spots, jnp.ones((), bf16), jnp.zeros((), bf16))


def place_low():
    return lax.broadcasted_iota(jnp.int32, (LANES, LANES), 0).astype(bf16)


def node_groups(node_ref):
    total = node_ref.shape[1]
    return jnp.concatenate(
        [node_ref[:, start : start + WIDE] for start in range(0, total, WIDE)], axis=0
    )


def sender_kernel(piece, extra, me_ref, node_ref, send_ref, edge_ref, weight_ref, vec_ref, *rest):
    pick_ref, base_ref, token_ref = rest[extra:]
    token_ref[...] = jnp.zeros_like(token_ref)
    width = edge_ref.shape[1]
    feat = edge_ref.shape[0]
    groups = node_ref.shape[1] // WIDE
    table = node_groups(node_ref)
    bias = spread(vec_ref[0], piece)
    for start in range(0, width, piece):
        ids = row_join(send_ref, start // LANES, piece // LANES)
        onehot = onehot_rows(ids & (WIDE - 1), WIDE)
        group = lax.shift_right_logical(ids, 8)
        found = dot(table, onehot)
        rows = found[:feat]
        for g in range(1, groups):
            rows = jnp.where(
                jnp.broadcast_to(group == g, (feat, piece)), found[g * feat : (g + 1) * feat], rows
            )
        low = rows.astype(bf16)
        pick_ref[:, start : start + piece] = low
        both = jnp.concatenate([low, edge_ref[:, start : start + piece]], axis=0)
        base_ref[:, start : start + piece] = dot(weight_ref[...], both) + bias


def gather_blocks(meta_ref, first, code_ref, start, count, source_ref):
    feat = source_ref.shape[0]
    parts = []
    for k in range(count):
        tile = meta_ref[first + start + k]
        code = code_ref[0, start + k : start + k + 1, :]
        index = jnp.broadcast_to(code & (LANES - 1), (feat, LANES))
        rows = source_ref[:, pl.ds(pl.multiple_of(tile * LANES, LANES), LANES)]
        taken = jnp.take_along_axis(rows, index, axis=1)
        parts.append(jnp.where(jnp.broadcast_to(code < LANES, (feat, LANES)), taken, 0.0))
    return jnp.concatenate(parts, axis=1)


def scatter_blocks(meta_ref, first, code_ref, start, count, values, total_ref, place):
    for k in range(count):
        tile = meta_ref[first + start + k]
        onehot = onehot_low(code_ref[0, start + k : start + k + 1, :], place)
        term = dot_nt(values[:, k * LANES : (k + 1) * LANES], onehot)
        where_to = pl.ds(pl.multiple_of(tile * LANES, LANES), LANES)
        total_ref[:, where_to] = total_ref[:, where_to] + term


def forward_kernel(masks, blocks, piece, extra, meta_ref, code_ref, base_ref, edge_ref, in_ref, out_ref, vec_ref, *rest):
    count = len(masks)
    shard_refs = rest[:count]
    result_ref, act_ref, slope_ref, normed_ref, inv_ref, token_ref = rest[count + extra : count + extra + 6]
    part_refs = rest[count + extra + 6 : -2]
    proj_ref, total_ref = rest[-2:]
    token_ref[...] = jnp.zeros_like(token_ref)
    step = pl.program_id(0)
    inner = pl.program_id(1)

    @pl.when(inner == 0)
    def _():
        for k in range(count):

            @pl.when(step == k)
            def _():
                proj_ref[...] = dot(in_ref[...], shard_refs[k][...])

        total_ref[...] = jnp.zeros_like(total_ref)

    width = edge_ref.shape[1]
    first = 1 + owner(masks, step, meta_ref) * blocks + inner * (width // LANES)
    per = piece // LANES
    place = place_low()
    for start in range(0, width, piece):
        lanes = slice(start, start + piece)
        block = start // LANES
        half = base_ref[:, lanes] + gather_blocks(meta_ref, first, code_ref, block, per, proj_ref)
        up = jnp.tanh(half) + 1.0
        act = half * up
        slope_ref[:, lanes] = (up + act * (2.0 - up)).astype(bf16)
        act_low = act.astype(bf16)
        act_ref[:, lanes] = act_low
        second = dot(out_ref[...], act_low) + spread(vec_ref[1], piece)
        centered = second - jnp.mean(second, axis=0, keepdims=True)
        inv = lax.rsqrt(jnp.mean(centered * centered, axis=0, keepdims=True) + epsilon)
        normed = centered * inv
        normed_ref[:, lanes] = normed.astype(bf16)
        for k in range(per):
            inv_ref[block + k : block + k + 1, :] = inv[:, k * LANES : (k + 1) * LANES]
        message = (normed * spread(vec_ref[2], piece) + spread(vec_ref[3], piece)).astype(bf16)
        result_ref[:, lanes] = edge_ref[:, lanes] + message
        scatter_blocks(meta_ref, first, code_ref, block, per, message, total_ref, place)

    @pl.when(inner == pl.num_programs(1) - 1)
    def _():
        low = total_ref[...].astype(bf16)
        for k in range(count):

            @pl.when(step == k)
            def _():
                part_refs[k][...] = low


def node_kernel(peers, node_ref, cot_ref, in_t_ref, in_ref, out_t_ref, out_ref, vec_ref, *rest):
    part_refs = rest[:peers]
    result_ref, base_ref, back_ref, pack_ref = rest[peers:]
    feat, total = node_ref.shape
    aggregate = part_refs[0][...].astype(f32)
    for k in range(1, peers):
        aggregate = aggregate + part_refs[k][...].astype(f32)
    node_inputs = jnp.concatenate([node_ref[...], aggregate.astype(bf16)], axis=0)
    pre = dot(in_t_ref[...], node_inputs) + spread(vec_ref[4], total)
    sig = sigmoid(pre)
    act = pre * sig
    slope = sig + act * (1.0 - sig)
    act_low = act.astype(bf16)
    second = dot(out_t_ref[...], act_low) + spread(vec_ref[5], total)
    centered = second - jnp.mean(second, axis=0, keepdims=True)
    inv = lax.rsqrt(jnp.mean(centered * centered, axis=0, keepdims=True) + epsilon)
    normed = centered * inv
    gain = spread(vec_ref[6], total)
    update = normed * gain + spread(vec_ref[7], total)
    result_ref[...] = (node_ref[...].astype(f32) + update).astype(bf16)
    upstream = cot_ref[...].astype(f32)
    scaled = upstream * gain
    inner = (
        scaled
        - jnp.mean(scaled, axis=0, keepdims=True)
        - normed * jnp.mean(scaled * normed, axis=0, keepdims=True)
    )
    grad = (inner * inv).astype(bf16)
    third = (dot(out_ref[...], grad) * slope).astype(bf16)
    input_grad = dot(in_ref[...], third)
    base_ref[...] = upstream + input_grad[:feat]
    back_ref[...] = input_grad[feat:].astype(bf16)
    pack_ref[...] = jnp.zeros_like(pack_ref)
    pack_ref[:feat, : 2 * feat] = dot_nt(third, node_inputs)
    pack_ref[:feat, 2 * feat : 3 * feat] = dot_nt(act_low, grad)
    ones = jnp.ones((8, LANES), f32)
    sums = (
        fold(third.astype(f32)),
        fold(grad.astype(f32)),
        fold(upstream * normed),
        fold(upstream),
    )
    for k in range(4):
        pack_ref[feat + k : feat + k + 1, :feat] = dot_nt_exact(ones, sums[k])[:1]


def backward_kernel(masks, blocks, piece, extra, meta_ref, code_ref, cot_ref, normed_ref, act_ref, slope_ref, inv_ref, edge_ref, pick_ref, out_ref, in_ref, vec_ref, *rest):
    count = len(masks)
    back_refs = rest[:count]
    shard_refs = rest[count : 2 * count]
    prior_refs = rest[2 * count : 2 * count + extra]
    grad_ref, first_ref, pack_ref, token_ref = rest[2 * count + extra : 2 * count + extra + 4]
    part_refs = rest[2 * count + extra + 4 : -6]
    pull_ref, total_ref, w1_ref, wr_ref, w2_ref, sum_ref = rest[-6:]
    step = pl.program_id(0)
    inner = pl.program_id(1)
    feat, width = edge_ref.shape
    token_ref[...] = jnp.zeros_like(token_ref)

    @pl.when((step == 0) & (inner == 0))
    def _():
        w1_ref[...] = jnp.zeros_like(w1_ref)
        wr_ref[...] = jnp.zeros_like(wr_ref)
        w2_ref[...] = jnp.zeros_like(w2_ref)
        sum_ref[...] = jnp.zeros_like(sum_ref)

    @pl.when(inner == 0)
    def _():
        for k in range(count):

            @pl.when(step == k)
            def _():
                pull_ref[...] = back_refs[k][...].astype(f32)

        total_ref[...] = jnp.zeros_like(total_ref)

    first = 1 + owner(masks, step, meta_ref) * blocks + inner * (width // LANES)
    per = piece // LANES
    place = place_low()
    for start in range(0, width, piece):
        lanes = slice(start, start + piece)
        block = start // LANES
        cot = cot_ref[:, lanes].astype(f32)
        upstream = cot + gather_blocks(meta_ref, first, code_ref, block, per, pull_ref)
        normed = normed_ref[:, lanes].astype(f32)
        scaled = upstream * spread(vec_ref[2], piece)
        inner_grad = (
            scaled
            - jnp.mean(scaled, axis=0, keepdims=True)
            - normed * jnp.mean(scaled * normed, axis=0, keepdims=True)
        )
        second = (inner_grad * row_join(inv_ref, block, per)).astype(bf16)
        sum_ref[2] += fold(upstream * normed)
        sum_ref[3] += fold(upstream)
        sum_ref[1] += fold(second.astype(f32))
        w2_ref[...] += dot_nt(act_ref[:, lanes], second)
        grad = (dot(out_ref[...], second) * slope_ref[:, lanes].astype(f32)).astype(bf16)
        first_ref[:, lanes] = grad
        sum_ref[0] += fold(grad.astype(f32))
        grad_ref[:, lanes] = cot + dot(in_ref[...], grad)
        both = jnp.concatenate([pick_ref[:, lanes], edge_ref[:, lanes]], axis=0)
        w1_ref[...] += dot_nt(grad, both)
        scatter_blocks(meta_ref, first, code_ref, block, per, grad, total_ref, place)
    last = inner == pl.num_programs(1) - 1

    @pl.when(last)
    def _():
        low = total_ref[...].astype(bf16)
        for k in range(count):

            @pl.when(step == k)
            def _():
                part_refs[k][...] = low
                wr_ref[...] += dot_nt(low, shard_refs[k][...])

    @pl.when(last & (step == pl.num_programs(0) - 1))
    def _():
        pack_ref[...] = jnp.zeros_like(pack_ref)
        pack_ref[:feat, :feat] = w1_ref[:, :feat]
        pack_ref[:feat, feat : 2 * feat] = wr_ref[...]
        pack_ref[:feat, 2 * feat : 3 * feat] = w1_ref[:, feat:]
        pack_ref[:feat, 3 * feat : 4 * feat] = w2_ref[...]
        ones = jnp.ones((8, LANES), f32)
        for k in range(4):
            pack_ref[feat + k : feat + k + 1, :feat] = dot_nt_exact(ones, sum_ref[k])[:1]
        if extra:
            pack_ref[...] += prior_refs[2][...]


def sender_sum_kernel(grad_ref, send_ref, sum_ref, token_ref, total_ref):
    feat, width = grad_ref.shape
    groups = sum_ref.shape[1] // WIDE
    step = pl.program_id(0)
    token_ref[...] = jnp.zeros_like(token_ref)

    @pl.when(step == 0)
    def _():
        total_ref[...] = jnp.zeros_like(total_ref)

    ids = row_join(send_ref, 0, width // LANES)
    onehot = onehot_rows(ids & (WIDE - 1), WIDE)
    group = jnp.broadcast_to(lax.shift_right_logical(ids, 8).astype(bf16), (feat, width))
    values = grad_ref[...]
    zero = jnp.zeros((), bf16)
    masked = jnp.concatenate(
        [jnp.where(group == jnp.asarray(g, bf16), values, zero) for g in range(groups)], axis=0
    )
    total_ref[...] += dot_nt(masked, onehot)

    @pl.when(step == pl.num_programs(0) - 1)
    def _():
        for g in range(groups):
            sum_ref[:, g * WIDE : (g + 1) * WIDE] = total_ref[g * feat : (g + 1) * feat, :]


def finish_kernel(sums, peers, base_ref, weight_ref, pack_ref, *rest):
    sum_refs = rest[:sums]
    part_refs = rest[sums : sums + peers]
    grad_ref, e1, b1, e2, b2, g1, s1, n1, c1, n2, c2, g2, s2 = rest[sums + peers :]
    sent = sum_refs[0][...]
    for k in range(1, sums):
        sent = sent + sum_refs[k][...]
    total = part_refs[0][...].astype(f32)
    for k in range(1, peers):
        total = total + part_refs[k][...].astype(f32)
    both = jnp.concatenate([sent, total], axis=0)
    grad_ref[...] = base_ref[...] + dot_exact(weight_ref[...], both)
    feat = base_ref.shape[0]
    e1[...] = pack_ref[:feat, : 3 * feat]
    e2[...] = pack_ref[:feat, 3 * feat : 4 * feat]
    n1[...] = pack_ref[:feat, 4 * feat : 6 * feat]
    n2[...] = pack_ref[:feat, 6 * feat : 7 * feat]
    for k, ref in enumerate((b1, b2, g1, s1)):
        ref[...] = pack_ref[feat + k : feat + k + 1, :feat]
    for k, ref in enumerate((c1, c2, g2, s2)):
        ref[...] = pack_ref[feat + k : feat + k + 1, 4 * feat : 5 * feat]


def owner(masks, step, meta_ref):
    stride = masks[1] - masks[0] if len(masks) > 1 else 0
    return meta_ref[0] ^ (masks[0] + stride * step)


def flip(value):
    size = value.shape[1]
    rows = lax.broadcasted_iota(jnp.int32, (size, size), 0)
    cols = lax.broadcasted_iota(jnp.int32, (size, size), 1)
    eye = jnp.where(rows == cols, 1.0, 0.0).astype(bf16)
    return dot_nt(eye, value).astype(value.dtype)


def prepare_kernel(in_ref, out_ref, node_in_ref, node_out_ref, *rest):
    row_refs = rest[:8]
    vec_ref, se_ref, re_ref, out_t_ref, back_ref, edge_back_ref, node_back_ref, node_out_t_ref, sr_ref = rest[8:]
    feat = out_ref.shape[0]
    rows = lax.broadcasted_iota(jnp.int32, (feat, feat), 0)
    cols = lax.broadcasted_iota(jnp.int32, (feat, feat), 1)
    for k in range(8):
        spot = jnp.where(rows == cols, jnp.broadcast_to(row_refs[k][...], (feat, feat)), 0.0)
        column = jnp.sum(spot, axis=1, keepdims=True)
        vec_ref[k] = jnp.broadcast_to(column * 0.5 if k == 0 else column, (feat, LANES))
    half = jnp.asarray(0.5, bf16)
    sent = in_ref[:, :feat]
    received = in_ref[:, feat : 2 * feat]
    edge = in_ref[:, 2 * feat :]
    se_ref[...] = jnp.concatenate([sent, edge], axis=1) * half
    re_ref[...] = received * half
    out_t_ref[...] = flip(out_ref[...])
    back_ref[...] = out_ref[...] * half
    edge_back_ref[...] = flip(edge)
    node_back_ref[:feat] = flip(node_in_ref[:, :feat])
    node_back_ref[feat:] = flip(node_in_ref[:, feat:])
    node_out_t_ref[...] = flip(node_out_ref[...])
    sr_ref[...] = jnp.concatenate([flip(sent), flip(received)], axis=1).astype(f32)


def struct(shape, dtype):
    return jax.ShapeDtypeStruct(shape, dtype)


def whole(shape):
    return pl.BlockSpec(shape, lambda *_: (0,) * len(shape))


def per_device(groups, peers, *arrays):
    (
        nodes, edges, send_nodes, block_tile, block_count, slot_ids,
        edge_in_weight, edge_in_bias, edge_out_weight, edge_out_bias, edge_gain, edge_shift,
        node_in_weight, node_in_bias, node_out_weight, node_out_bias, node_gain, node_shift,
        node_cot, edge_cot,
    ) = arrays
    feat = nodes.shape[1]
    node_total = nodes.shape[0]
    edge_total = edges.shape[0]
    block_total = block_tile.shape[0]
    blocks = block_total // peers
    per_peer = edge_total // peers
    rows = edge_total // LANES

    def swap(value, mask):
        if mask == 0:
            return value
        return lax.ppermute(value, "peer", [(i, i ^ mask) for i in range(peers)])

    near = [m for m in range(0, peers, 2)]
    routed = [m for m in (4, 6, 2) if m < peers] + [m for m in range(8, peers, 2)]

    def tie(value, *others):
        return lax.optimization_barrier((value,) + others)[0]

    def gather_first(value):
        return {m: swap(value, m) for m in [0, 1] + routed}

    def gather_rest(found, gate):
        for m in routed:
            found[m | 1] = swap(tie(found[m], gate), 1)
        return found

    def swap_near(parts):
        return {m: swap(parts[m | 1], 1) for m in routed + [0]}

    def sum_out(parts, got):
        sums = [parts[0], got[0]]
        for m in routed:
            both = (parts[m].astype(f32) + got[m].astype(f32)).astype(bf16)
            sums.append(both)
        return sums[:2] + [swap(both, m) for both, m in zip(sums[2:], routed)], sums[-1]

    def add_groups(value):
        if groups > 4:
            mask = 1
            while mask < groups:
                value = value + lax.ppermute(value, "grp", [(i, i ^ mask) for i in range(groups)])
                mask *= 2
            return value
        others = [lax.ppermute(value, "grp", [(i, i ^ mask) for i in range(groups)]) for mask in range(1, groups)]
        return sum(others, value)

    def add_far(value):
        if peers > 8:
            mask = 2
            while mask < peers:
                value = value + swap(value, mask)
                mask *= 2
            return value
        return sum([swap(value, m) for m in routed], value)

    halves = [tuple(range(0, peers, 2)), tuple(range(1, peers, 2))]
    send_teams = halves
    quarter = (peers + 3) // 4
    teams = [halves[0][:quarter], halves[1], halves[0][quarter:]]
    teams = [masks for masks in teams if masks]
    back_teams = [(0, 1), (2, 3)][: (peers + 3) // 4]
    for m in range(4, peers, 4):
        back_teams += [(m, m + 2), (m + 1, m + 3)]

    node_t = nodes.T
    edge_t = edges.T
    node_cot_t = node_cot.T
    edge_cot_t = edge_cot.T
    in_t = edge_in_weight.T
    send = send_nodes.reshape(rows, LANES)
    me = lax.axis_index("peer").astype(jnp.int32)[None]

    shards = gather_first(node_t)

    square = struct((feat, feat), bf16)
    vec, se_weight, re_weight, out_t, back_weight, edge_back, node_back, node_out_t, sr_weight = pl.pallas_call(
        prepare_kernel,
        out_shape=[
            struct((8, feat, LANES), f32), struct((feat, 2 * feat), bf16), square, square, square, square,
            struct((2 * feat, feat), bf16), square, struct((feat, 2 * feat), f32),
        ],
        name="prepare",
    )(
        in_t, edge_out_weight, node_in_weight.T, node_out_weight,
        *[v[None] for v in (edge_in_bias, edge_out_bias, edge_gain, edge_shift, node_in_bias, node_out_bias, node_gain, node_shift)],
    )

    wide = min(4096, per_peer)
    chunks = per_peer // wide
    sub = wide // LANES
    piece = min(1024, wide)

    def slab_of(masks):
        return pl.BlockSpec((feat, wide), lambda i, j, ref: (0, owner(masks, i, ref) * chunks + j))

    def rows_of(masks):
        return pl.BlockSpec((sub, LANES), lambda i, j, ref: (owner(masks, i, ref) * chunks + j, 0))

    def code_of(masks):
        return pl.BlockSpec((1, sub, LANES), lambda i, j, ref: (owner(masks, i, ref), j, 0))

    def kept_slab(place):
        return pl.BlockSpec((feat, wide), lambda i, j, ref: (0, (place + i) * chunks + j))

    own_slab = kept_slab(0)
    own_rows = pl.BlockSpec((sub, LANES), lambda i, j, ref: (i * chunks + j, 0))
    shard_spec = whole((feat, node_total))
    keep_spec = pl.BlockSpec(memory_space=pl.ANY)

    token = struct((8, LANES), f32)
    token_spec = whole((8, LANES))
    slab_shape = struct((feat, edge_total), bf16)
    shard_shape = struct((feat, node_total), bf16)
    chain = []
    for masks in send_teams:
        count = len(masks)
        extra = len(chain)
        pick, base, gate = pl.pallas_call(
            functools.partial(sender_kernel, min(512, wide), extra),
            grid_spec=pltpu.PrefetchScalarGridSpec(
                num_scalar_prefetch=1,
                grid=(count, chunks),
                in_specs=[shard_spec, rows_of(masks), slab_of(masks), whole((feat, 2 * feat)), whole((8, feat, LANES))] + [keep_spec] * extra,
                out_specs=[slab_of(masks), slab_of(masks), token_spec],
            ),
            out_shape=[slab_shape, struct((feat, edge_total), f32), token],
            input_output_aliases={6 + k: k for k in range(extra)},
            compiler_params=params(),
            name="sender",
        )(me, node_t, send, edge_t, se_weight, vec, *chain)
        if not chain:
            shards = gather_rest(shards, gate)
            send = tie(send, *[shards[m] for m in routed])
            live = jnp.arange(LANES, dtype=jnp.int32)[None, :] < tie(block_count, gate, *[shards[m] for m in routed])[:, None]
            code = slot_ids.reshape(block_total, LANES) + jnp.where(live, 0, LANES) + 2 * LANES * block_tile[:, None]
            code = lax.all_to_all(code, "peer", 0, 0, tiled=True)
            meta = jnp.concatenate([me, code[:, 0] // (2 * LANES)])
            code = (code & (2 * LANES - 1)).reshape(peers, blocks, LANES)
        chain = [pick, base]

    parts = {}
    chain = []
    for masks in teams:
        count = len(masks)
        extra = len(chain)
        *outs, = pl.pallas_call(
            functools.partial(forward_kernel, masks, blocks, piece, extra),
            grid_spec=pltpu.PrefetchScalarGridSpec(
                num_scalar_prefetch=1,
                grid=(count, chunks),
                in_specs=[code_of(masks), slab_of(masks), slab_of(masks), whole((feat, feat)), whole((feat, feat)), whole((8, feat, LANES))]
                + [shard_spec] * count
                + [keep_spec] * extra,
                out_specs=[slab_of(masks)] * 4 + [rows_of(masks), token_spec] + [shard_spec] * count,
                scratch_shapes=[pltpu.VMEM((feat, node_total), f32), pltpu.VMEM((feat, node_total), f32)],
            ),
            out_shape=[slab_shape] * 4 + [struct((rows, LANES), f32), token] + [shard_shape] * count,
            input_output_aliases={7 + count + k: k for k in range(extra)},
            compiler_params=params(),
            name="forward",
        )(meta, code, base, edge_t, re_weight, out_t, vec, *[shards[m] for m in masks], *chain)
        chain = outs[:5]
        parts.update(zip(masks, outs[6:]))
    result, act, slope, normed, inv = chain
    edge_result = result

    sums, _ = sum_out(parts, swap_near(parts))
    node_result, node_base, back, node_pack = pl.pallas_call(
        functools.partial(node_kernel, len(sums)),
        out_shape=[
            struct((feat, node_total), bf16),
            struct((feat, node_total), f32),
            struct((feat, node_total), bf16),
            struct((feat + 8, 4 * feat), f32),
        ],
        compiler_params=params(),
        name="node",
    )(node_t, node_cot_t, node_in_weight.T, node_back, node_out_t, node_out_weight, vec, *sums)

    near_pack = swap(node_pack, 1)
    backs = gather_first(back)

    parts = {}
    chain = []
    for masks in back_teams:
        count = len(masks)
        extra = len(chain)
        if masks == back_teams[-1] and extra:
            chain[2] = tie(chain[2], node_sum)
        *outs, = pl.pallas_call(
            functools.partial(backward_kernel, masks, blocks, piece, extra),
            grid_spec=pltpu.PrefetchScalarGridSpec(
                num_scalar_prefetch=1,
                grid=(count, chunks),
                in_specs=[code_of(masks)] + [slab_of(masks)] * 4 + [rows_of(masks)] + [slab_of(masks)] * 2
                + [whole((feat, feat)), whole((feat, feat)), whole((8, feat, LANES))]
                + [shard_spec] * (2 * count)
                + ([keep_spec] * 2 + [whole((feat + 8, 4 * feat))] if extra else []),
                out_specs=[slab_of(masks), slab_of(masks), whole((feat + 8, 4 * feat)), token_spec] + [shard_spec] * count,
                scratch_shapes=[
                    pltpu.VMEM((feat, node_total), f32),
                    pltpu.VMEM((feat, node_total), f32),
                    pltpu.VMEM((feat, 2 * feat), f32),
                    pltpu.VMEM((feat, feat), f32),
                    pltpu.VMEM((feat, feat), f32),
                    pltpu.VMEM((4, feat, LANES), f32),
                ],
            ),
            out_shape=[
                struct((feat, edge_total), f32),
                slab_shape,
                struct((feat + 8, 4 * feat), f32),
                token,
            ]
            + [shard_shape] * count,
            input_output_aliases={12 + 2 * count + k: k for k in range(2 if extra else 0)},
            compiler_params=params(),
            name="backward",
        )(
            meta, code, edge_cot_t, normed, act, slope, inv, edge_t, pick, back_weight, edge_back, vec,
            *[backs[m] for m in masks], *[shards[m] for m in masks], *chain,
        )
        chain, gate = outs[:3], outs[3]
        parts.update(zip(masks, outs[4:]))
        if not extra:
            backs = gather_rest(backs, gate)
            node_sum = node_pack + near_pack
        elif masks == back_teams[1]:
            node_sum = add_far(tie(node_sum, gate))
    edge_grad, first_grad, edge_pack = chain

    near_pack = swap(edge_pack, 1)
    got = swap_near(parts)

    sent, gates = [], []
    sum_wide = min(2048, per_peer)
    steps = edge_total // sum_wide // 2
    for start in (0, steps):
        if gates:
            got = {m: tie(value, gates[0]) for m, value in got.items()}
            sums, mark = sum_out(parts, got)
            edge_pack = add_far(tie(edge_pack + tie(near_pack, gates[0]), mark))
            first_grad = tie(first_grad, mark)
        total, gate = pl.pallas_call(
            sender_sum_kernel,
            grid=(steps,),
            in_specs=[
                pl.BlockSpec((feat, sum_wide), lambda i, start=start: (0, start + i)),
                pl.BlockSpec((sum_wide // LANES, LANES), lambda i, start=start: (start + i, 0)),
            ],
            out_specs=[shard_spec, token_spec],
            out_shape=[struct((feat, node_total), f32), token],
            scratch_shapes=[pltpu.VMEM((node_total // WIDE * feat, WIDE), f32)],
            compiler_params=params(),
            name="sender_sum",
        )(first_grad, send)
        sent.append(total)
        gates.append(gate)

    both_packs = add_groups(jnp.concatenate([tie(edge_pack, gates[1]), node_sum], axis=1))
    vec_out = struct((1, feat), f32)
    node_grad, e1, b1, e2, b2, g1, s1, n1, c1, n2, c2, g2, s2 = pl.pallas_call(
        functools.partial(finish_kernel, len(sent), len(sums)),
        out_shape=[
            struct((feat, node_total), f32),
            struct((feat, 3 * feat), f32), vec_out, struct((feat, feat), f32), vec_out, vec_out, vec_out,
            struct((feat, 2 * feat), f32), vec_out, struct((feat, feat), f32), vec_out, vec_out, vec_out,
        ],
        compiler_params=params(),
        name="finish",
    )(node_base, sr_weight, both_packs, *sent, *sums)

    def flat(row):
        return row.reshape(feat)

    return (
        node_result.T, edge_result.T, node_grad.T, edge_grad.T,
        e1.T, flat(b1), e2, flat(b2), flat(g1), flat(s1),
        n1.T, flat(c1), n2, flat(c2), flat(g2), flat(s2),
    )


def solution(mesh):
    split = P(("grp", "peer"), None)
    line = P(("grp", "peer"))
    one = P()
    return jax.shard_map(
        functools.partial(per_device, mesh.shape["grp"], mesh.shape["peer"]),
        mesh=mesh,
        in_specs=(split, split, line, line, line, line) + (one,) * 12 + (split, split),
        out_specs=(split, split, split, split) + (one,) * 12,
        check_vma=False,
    )
```

```python
import functools

import jax
import jax.numpy as jnp
from jax import lax
from jax.experimental import pallas as pl
from jax.experimental.pallas import tpu as pltpu
from jax.sharding import PartitionSpec as P

epsilon = 1e-05
bf16 = jnp.bfloat16
f32 = jnp.float32
LANES = 128
WIDE = 256


def dot(left, right):
    return jnp.dot(left, right, preferred_element_type=f32)


def dot_nt(left, right):
    return lax.dot_general(left, right, (((1,), (1,)), ((), ())), preferred_element_type=f32)


def dot_exact(left, right):
    return jnp.dot(left, right, preferred_element_type=f32, precision=lax.Precision.HIGHEST)


def dot_nt_exact(left, right):
    return lax.dot_general(
        left,
        right,
        (((1,), (1,)), ((), ())),
        preferred_element_type=f32,
        precision=lax.Precision.HIGHEST,
    )


def params(limit=48):
    return pltpu.CompilerParams(vmem_limit_bytes=limit * 1024 * 1024)


def spread(column, width):
    return jnp.concatenate([column] * (width // LANES), axis=1)


def fold(values):
    total = values[:, :LANES]
    for start in range(LANES, values.shape[1], LANES):
        total = total + values[:, start : start + LANES]
    return total


def row_join(ref, first, count):
    return jnp.concatenate([ref[first + k : first + k + 1, :] for k in range(count)], axis=1)


def sigmoid(values):
    return 0.5 * jnp.tanh(0.5 * values) + 0.5


def onehot_rows(row, rows):
    width = row.shape[1]
    place = lax.broadcasted_iota(jnp.int32, (rows, width), 0)
    return jnp.where(place == row, 1.0, 0.0).astype(bf16)


def onehot_low(row, place):
    spots = jnp.broadcast_to(row.astype(bf16), place.shape)
    return jnp.where(place == spots, jnp.ones((), bf16), jnp.zeros((), bf16))


def place_low():
    return lax.broadcasted_iota(jnp.int32, (LANES, LANES), 0).astype(bf16)


def node_groups(node_ref):
    total = node_ref.shape[1]
    return jnp.concatenate(
        [node_ref[:, start : start + WIDE] for start in range(0, total, WIDE)], axis=0
    )


def sender_kernel(piece, extra, me_ref, node_ref, send_ref, edge_ref, weight_ref, vec_ref, *rest):
    pick_ref, base_ref, token_ref = rest[extra:]
    token_ref[...] = jnp.zeros_like(token_ref)
    width = edge_ref.shape[1]
    feat = edge_ref.shape[0]
    groups = node_ref.shape[1] // WIDE
    table = node_groups(node_ref)
    bias = spread(vec_ref[0], piece)
    place = lax.broadcasted_iota(jnp.int32, (WIDE, piece), 0).astype(bf16)
    for start in range(0, width, piece):
        ids = row_join(send_ref, start // LANES, piece // LANES)
        onehot = onehot_low(ids & (WIDE - 1), place)
        group = lax.shift_right_logical(ids, 8)
        found = dot(table, onehot)
        rows = found[:feat]
        for g in range(1, groups):
            rows = jnp.where(
                jnp.broadcast_to(group == g, (feat, piece)), found[g * feat : (g + 1) * feat], rows
            )
        low = rows.astype(bf16)
        pick_ref[:, start : start + piece] = low
        both = jnp.concatenate([low, edge_ref[:, start : start + piece]], axis=0)
        base_ref[:, start : start + piece] = dot(weight_ref[...], both) + bias


def gather_blocks(meta_ref, first, code_ref, start, count, source_ref):
    feat = source_ref.shape[0]
    parts = []
    for k in range(count):
        tile = meta_ref[first + start + k]
        code = code_ref[0, start + k : start + k + 1, :]
        index = jnp.broadcast_to(code & (LANES - 1), (feat, LANES))
        rows = source_ref[:, pl.ds(pl.multiple_of(tile * LANES, LANES), LANES)]
        taken = jnp.take_along_axis(rows, index, axis=1)
        parts.append(jnp.where(jnp.broadcast_to(code < LANES, (feat, LANES)), taken, 0.0))
    return jnp.concatenate(parts, axis=1)


def scatter_blocks(meta_ref, first, code_ref, start, count, values, total_ref, place):
    for k in range(count):
        tile = meta_ref[first + start + k]
        onehot = onehot_low(code_ref[0, start + k : start + k + 1, :], place)
        term = dot_nt(values[:, k * LANES : (k + 1) * LANES], onehot)
        where_to = pl.ds(pl.multiple_of(tile * LANES, LANES), LANES)
        total_ref[:, where_to] = total_ref[:, where_to] + term


def forward_kernel(masks, blocks, piece, extra, meta_ref, code_ref, base_ref, edge_ref, in_ref, out_ref, vec_ref, *rest):
    count = len(masks)
    shard_refs = rest[:count]
    result_ref, act_ref, slope_ref, normed_ref, inv_ref, token_ref = rest[count + extra : count + extra + 6]
    part_refs = rest[count + extra + 6 : -2]
    proj_ref, total_ref = rest[-2:]
    token_ref[...] = jnp.zeros_like(token_ref)
    step = pl.program_id(0)
    inner = pl.program_id(1)

    @pl.when(inner == 0)
    def _():
        for k in range(count):

            @pl.when(step == k)
            def _():
                proj_ref[...] = dot(in_ref[...], shard_refs[k][...])

        total_ref[...] = jnp.zeros_like(total_ref)

    width = edge_ref.shape[1]
    first = 1 + owner(masks, step, meta_ref) * blocks + inner * (width // LANES)
    per = piece // LANES
    place = place_low()
    for start in range(0, width, piece):
        lanes = slice(start, start + piece)
        block = start // LANES
        half = base_ref[:, lanes] + gather_blocks(meta_ref, first, code_ref, block, per, proj_ref)
        up = jnp.tanh(half) + 1.0
        act = half * up
        slope_ref[:, lanes] = (up + act * (2.0 - up)).astype(bf16)
        act_low = act.astype(bf16)
        act_ref[:, lanes] = act_low
        second = dot(out_ref[...], act_low) + spread(vec_ref[1], piece)
        centered = second - jnp.mean(second, axis=0, keepdims=True)
        inv = lax.rsqrt(jnp.mean(centered * centered, axis=0, keepdims=True) + epsilon)
        normed = centered * inv
        normed_ref[:, lanes] = normed.astype(bf16)
        for k in range(per):
            inv_ref[block + k : block + k + 1, :] = inv[:, k * LANES : (k + 1) * LANES]
        message = (normed * spread(vec_ref[2], piece) + spread(vec_ref[3], piece)).astype(bf16)
        result_ref[:, lanes] = edge_ref[:, lanes] + message
        scatter_blocks(meta_ref, first, code_ref, block, per, message, total_ref, place)

    @pl.when(inner == pl.num_programs(1) - 1)
    def _():
        low = total_ref[...].astype(bf16)
        for k in range(count):

            @pl.when(step == k)
            def _():
                part_refs[k][...] = low


def node_kernel(peers, node_ref, cot_ref, in_t_ref, in_ref, out_t_ref, out_ref, vec_ref, *rest):
    part_refs = rest[:peers]
    result_ref, base_ref, back_ref, pack_ref = rest[peers:]
    feat, total = node_ref.shape
    aggregate = part_refs[0][...].astype(f32)
    for k in range(1, peers):
        aggregate = aggregate + part_refs[k][...].astype(f32)
    node_inputs = jnp.concatenate([node_ref[...], aggregate.astype(bf16)], axis=0)
    pre = dot(in_t_ref[...], node_inputs) + spread(vec_ref[4], total)
    sig = sigmoid(pre)
    act = pre * sig
    slope = sig + act * (1.0 - sig)
    act_low = act.astype(bf16)
    second = dot(out_t_ref[...], act_low) + spread(vec_ref[5], total)
    centered = second - jnp.mean(second, axis=0, keepdims=True)
    inv = lax.rsqrt(jnp.mean(centered * centered, axis=0, keepdims=True) + epsilon)
    normed = centered * inv
    gain = spread(vec_ref[6], total)
    update = normed * gain + spread(vec_ref[7], total)
    result_ref[...] = (node_ref[...].astype(f32) + update).astype(bf16)
    upstream = cot_ref[...].astype(f32)
    scaled = upstream * gain
    inner = (
        scaled
        - jnp.mean(scaled, axis=0, keepdims=True)
        - normed * jnp.mean(scaled * normed, axis=0, keepdims=True)
    )
    grad = (inner * inv).astype(bf16)
    third = (dot(out_ref[...], grad) * slope).astype(bf16)
    input_grad = dot(in_ref[...], third)
    base_ref[...] = upstream + input_grad[:feat]
    back_ref[...] = input_grad[feat:].astype(bf16)
    pack_ref[...] = jnp.zeros_like(pack_ref)
    pack_ref[:feat, 4 * feat : 6 * feat] = dot_nt(third, node_inputs)
    pack_ref[:feat, 6 * feat : 7 * feat] = dot_nt(act_low, grad)
    ones = jnp.ones((8, LANES), f32)
    sums = (
        fold(third.astype(f32)),
        fold(grad.astype(f32)),
        fold(upstream * normed),
        fold(upstream),
    )
    for k in range(4):
        pack_ref[feat + k : feat + k + 1, 4 * feat : 5 * feat] = dot_nt_exact(ones, sums[k])[:1]


def backward_kernel(masks, blocks, piece, extra, meta_ref, code_ref, cot_ref, normed_ref, act_ref, slope_ref, inv_ref, edge_ref, pick_ref, out_ref, in_ref, vec_ref, *rest):
    count = len(masks)
    back_refs = rest[:count]
    shard_refs = rest[count : 2 * count]
    prior_refs = rest[2 * count : 2 * count + extra]
    grad_ref, first_ref, pack_ref, token_ref = rest[2 * count + extra : 2 * count + extra + 4]
    part_refs = rest[2 * count + extra + 4 : -6]
    pull_ref, total_ref, w1_ref, wr_ref, w2_ref, sum_ref = rest[-6:]
    step = pl.program_id(0)
    inner = pl.program_id(1)
    feat, width = edge_ref.shape
    token_ref[...] = jnp.zeros_like(token_ref)

    @pl.when((step == 0) & (inner == 0))
    def _():
        w1_ref[...] = jnp.zeros_like(w1_ref)
        wr_ref[...] = jnp.zeros_like(wr_ref)
        w2_ref[...] = jnp.zeros_like(w2_ref)
        sum_ref[...] = jnp.zeros_like(sum_ref)

    @pl.when(inner == 0)
    def _():
        for k in range(count):

            @pl.when(step == k)
            def _():
                pull_ref[...] = back_refs[k][...].astype(f32)

        total_ref[...] = jnp.zeros_like(total_ref)

    first = 1 + owner(masks, step, meta_ref) * blocks + inner * (width // LANES)
    per = piece // LANES
    place = place_low()
    for start in range(0, width, piece):
        lanes = slice(start, start + piece)
        block = start // LANES
        cot = cot_ref[:, lanes].astype(f32)
        upstream = cot + gather_blocks(meta_ref, first, code_ref, block, per, pull_ref)
        normed = normed_ref[:, lanes].astype(f32)
        scaled = upstream * spread(vec_ref[2], piece)
        inner_grad = (
            scaled
            - jnp.mean(scaled, axis=0, keepdims=True)
            - normed * jnp.mean(scaled * normed, axis=0, keepdims=True)
        )
        second = (inner_grad * row_join(inv_ref, block, per)).astype(bf16)
        sum_ref[2] += fold(upstream * normed)
        sum_ref[3] += fold(upstream)
        sum_ref[1] += fold(second.astype(f32))
        w2_ref[...] += dot_nt(act_ref[:, lanes], second)
        grad = (dot(out_ref[...], second) * slope_ref[:, lanes].astype(f32)).astype(bf16)
        first_ref[:, lanes] = grad
        sum_ref[0] += fold(grad.astype(f32))
        grad_ref[:, lanes] = cot + dot(in_ref[...], grad)
        both = jnp.concatenate([pick_ref[:, lanes], edge_ref[:, lanes]], axis=0)
        w1_ref[...] += dot_nt(grad, both)
        scatter_blocks(meta_ref, first, code_ref, block, per, grad, total_ref, place)
    last = inner == pl.num_programs(1) - 1

    @pl.when(last)
    def _():
        low = total_ref[...].astype(bf16)
        for k in range(count):

            @pl.when(step == k)
            def _():
                part_refs[k][...] = low
                wr_ref[...] += dot_nt(low, shard_refs[k][...])

    @pl.when(last & (step == pl.num_programs(0) - 1))
    def _():
        pack_ref[...] = jnp.zeros_like(pack_ref)
        pack_ref[:feat, :feat] = w1_ref[:, :feat]
        pack_ref[:feat, feat : 2 * feat] = wr_ref[...]
        pack_ref[:feat, 2 * feat : 3 * feat] = w1_ref[:, feat:]
        pack_ref[:feat, 3 * feat : 4 * feat] = w2_ref[...]
        ones = jnp.ones((8, LANES), f32)
        for k in range(4):
            pack_ref[feat + k : feat + k + 1, :feat] = dot_nt_exact(ones, sum_ref[k])[:1]
        pack_ref[...] += prior_refs[0][...]


def sender_sum_kernel(starts, me_ref, send_ref, *rest):
    grad_refs = rest[: len(starts)]
    sum_ref, token_ref, total_ref, grad_ref = rest[len(starts) :]
    feat, width = grad_ref.shape
    groups = sum_ref.shape[1] // WIDE
    step = pl.program_id(0)
    token_ref[...] = jnp.zeros_like(token_ref)
    for k, start in enumerate(starts):
        after = starts[k + 1] if k + 1 < len(starts) else pl.num_programs(0)

        @pl.when((step >= start) & (step < after))
        def _():
            grad_ref[...] = grad_refs[k][...]

    @pl.when(step == 0)
    def _():
        total_ref[...] = jnp.zeros_like(total_ref)

    ids = row_join(send_ref, 0, width // LANES)
    onehot = onehot_rows(ids & (WIDE - 1), WIDE)
    group = jnp.broadcast_to(lax.shift_right_logical(ids, 8).astype(bf16), (feat, width))
    values = grad_ref[...]
    zero = jnp.zeros((), bf16)
    masked = jnp.concatenate(
        [jnp.where(group == jnp.asarray(g, bf16), values, zero) for g in range(groups)], axis=0
    )
    total_ref[...] += dot_nt(masked, onehot)

    @pl.when(step == pl.num_programs(0) - 1)
    def _():
        for g in range(groups):
            sum_ref[:, g * WIDE : (g + 1) * WIDE] = total_ref[g * feat : (g + 1) * feat, :]


def finish_kernel(sums, peers, base_ref, weight_ref, pack_ref, *rest):
    sum_refs = rest[:sums]
    part_refs = rest[sums : sums + peers]
    grad_ref, e1, b1, e2, b2, g1, s1, n1, c1, n2, c2, g2, s2 = rest[sums + peers :]
    sent = sum_refs[0][...]
    for k in range(1, sums):
        sent = sent + sum_refs[k][...]
    total = part_refs[0][...].astype(f32)
    for k in range(1, peers):
        total = total + part_refs[k][...].astype(f32)
    both = jnp.concatenate([sent, total], axis=0)
    grad_ref[...] = base_ref[...] + dot_exact(weight_ref[...], both)
    feat = base_ref.shape[0]
    e1[...] = pack_ref[:feat, : 3 * feat]
    e2[...] = pack_ref[:feat, 3 * feat : 4 * feat]
    n1[...] = pack_ref[:feat, 4 * feat : 6 * feat]
    n2[...] = pack_ref[:feat, 6 * feat : 7 * feat]
    for k, ref in enumerate((b1, b2, g1, s1)):
        ref[...] = pack_ref[feat + k : feat + k + 1, :feat]
    for k, ref in enumerate((c1, c2, g2, s2)):
        ref[...] = pack_ref[feat + k : feat + k + 1, 4 * feat : 5 * feat]


def owner(masks, step, meta_ref):
    stride = masks[1] - masks[0] if len(masks) > 1 else 0
    return meta_ref[0] ^ (masks[0] + stride * step)


def flip(value):
    size = value.shape[1]
    rows = lax.broadcasted_iota(jnp.int32, (size, size), 0)
    cols = lax.broadcasted_iota(jnp.int32, (size, size), 1)
    eye = jnp.where(rows == cols, 1.0, 0.0).astype(bf16)
    return dot_nt(eye, value).astype(value.dtype)


def prepare_kernel(in_ref, out_ref, node_in_ref, node_out_ref, *rest):
    row_refs = rest[:8]
    vec_ref, se_ref, re_ref, out_t_ref, back_ref, edge_back_ref, node_back_ref, node_out_t_ref, sr_ref = rest[8:]
    feat = out_ref.shape[0]
    rows = lax.broadcasted_iota(jnp.int32, (feat, feat), 0)
    cols = lax.broadcasted_iota(jnp.int32, (feat, feat), 1)
    for k in range(8):
        spot = jnp.where(rows == cols, jnp.broadcast_to(row_refs[k][...], (feat, feat)), 0.0)
        column = jnp.sum(spot, axis=1, keepdims=True)
        vec_ref[k] = jnp.broadcast_to(column * 0.5 if k == 0 else column, (feat, LANES))
    half = jnp.asarray(0.5, bf16)
    sent = in_ref[:, :feat]
    received = in_ref[:, feat : 2 * feat]
    edge = in_ref[:, 2 * feat :]
    se_ref[...] = jnp.concatenate([sent, edge], axis=1) * half
    re_ref[...] = received * half
    out_t_ref[...] = flip(out_ref[...])
    back_ref[...] = out_ref[...] * half
    edge_back_ref[...] = flip(edge)
    node_back_ref[:feat] = flip(node_in_ref[:, :feat])
    node_back_ref[feat:] = flip(node_in_ref[:, feat:])
    node_out_t_ref[...] = flip(node_out_ref[...])
    sr_ref[...] = jnp.concatenate([flip(sent), flip(received)], axis=1).astype(f32)


def struct(shape, dtype):
    return jax.ShapeDtypeStruct(shape, dtype)


def whole(shape):
    return pl.BlockSpec(shape, lambda *_: (0,) * len(shape))


def per_device(groups, peers, *arrays):
    (
        nodes, edges, send_nodes, block_tile, block_count, slot_ids,
        edge_in_weight, edge_in_bias, edge_out_weight, edge_out_bias, edge_gain, edge_shift,
        node_in_weight, node_in_bias, node_out_weight, node_out_bias, node_gain, node_shift,
        node_cot, edge_cot,
    ) = arrays
    feat = nodes.shape[1]
    node_total = nodes.shape[0]
    edge_total = edges.shape[0]
    block_total = block_tile.shape[0]
    blocks = block_total // peers
    per_peer = edge_total // peers
    rows = edge_total // LANES

    def swap(value, mask):
        if mask == 0:
            return value
        return lax.ppermute(value, "peer", [(i, i ^ mask) for i in range(peers)])

    near = [m for m in range(0, peers, 2)]
    routed = [m for m in (4, 6, 2) if m < peers] + [m for m in range(8, peers, 2)]

    def tie(value, *others):
        return lax.optimization_barrier((value,) + others)[0]

    def gather_first(value):
        return {m: swap(value, m) for m in [0, 1] + routed}

    def gather_rest(found, gate):
        for m in routed:
            found[m | 1] = swap(tie(found[m], gate), 1)
        return found

    def join(parts, got, m):
        return (parts[m].astype(f32) + got[m].astype(f32)).astype(bf16)

    def add_groups(value):
        if groups > 4:
            mask = 1
            while mask < groups:
                value = value + lax.ppermute(value, "grp", [(i, i ^ mask) for i in range(groups)])
                mask *= 2
            return value
        others = [lax.ppermute(value, "grp", [(i, i ^ mask) for i in range(groups)]) for mask in range(1, groups)]
        return sum(others, value)

    halves = [tuple(range(0, peers, 2)), tuple(range(1, peers, 2))]
    firsts_of = list(range(0, peers, 4))
    pair = lambda m: (m, m + 2) if m + 2 < peers else (m,)
    teams = [pair(m + side) for m in firsts_of[::-1] for side in (1, 0)]
    back_teams = [pair(0)]
    for m in firsts_of[1:]:
        back_teams += [pair(m), pair(m + 1)]
    back_teams.append(pair(1))

    node_t = nodes.T
    edge_t = edges.T
    node_cot_t = node_cot.T
    edge_cot_t = edge_cot.T
    in_t = edge_in_weight.T
    send = send_nodes.reshape(rows, LANES)
    me = lax.axis_index("peer").astype(jnp.int32)[None]

    shards = gather_first(node_t)

    square = struct((feat, feat), bf16)
    vec, se_weight, re_weight, out_t, back_weight, edge_back, node_back, node_out_t, sr_weight = pl.pallas_call(
        prepare_kernel,
        out_shape=[
            struct((8, feat, LANES), f32), struct((feat, 2 * feat), bf16), square, square, square, square,
            struct((2 * feat, feat), bf16), square, struct((feat, 2 * feat), f32),
        ],
        name="prepare",
    )(
        in_t, edge_out_weight, node_in_weight.T, node_out_weight,
        *[v[None] for v in (edge_in_bias, edge_out_bias, edge_gain, edge_shift, node_in_bias, node_out_bias, node_gain, node_shift)],
    )

    wide = min(4096, per_peer)
    chunks = per_peer // wide
    sub = wide // LANES
    piece = min(2048, wide)

    def slab_of(masks):
        return pl.BlockSpec((feat, wide), lambda i, j, ref: (0, owner(masks, i, ref) * chunks + j))

    def rows_of(masks):
        return pl.BlockSpec((sub, LANES), lambda i, j, ref: (owner(masks, i, ref) * chunks + j, 0))

    def code_of(masks):
        return pl.BlockSpec((1, sub, LANES), lambda i, j, ref: (owner(masks, i, ref), j, 0))

    def kept_slab(place):
        return pl.BlockSpec((feat, wide), lambda i, j, ref: (0, (place + i) * chunks + j))

    own_slab = kept_slab(0)
    own_rows = pl.BlockSpec((sub, LANES), lambda i, j, ref: (i * chunks + j, 0))
    shard_spec = whole((feat, node_total))
    keep_spec = pl.BlockSpec(memory_space=pl.ANY)

    token = struct((8, LANES), f32)
    token_spec = whole((8, LANES))
    slab_shape = struct((feat, edge_total), bf16)
    shard_shape = struct((feat, node_total), bf16)
    picks, bases = [], []
    for masks in halves:
        count = len(masks)
        pick, base, gate = pl.pallas_call(
            functools.partial(sender_kernel, min(1024, wide), 0),
            grid_spec=pltpu.PrefetchScalarGridSpec(
                num_scalar_prefetch=1,
                grid=(count, chunks),
                in_specs=[shard_spec, rows_of(masks), slab_of(masks), whole((feat, 2 * feat)), whole((8, feat, LANES))],
                out_specs=[own_slab, own_slab, token_spec],
            ),
            out_shape=[struct((feat, count * per_peer), bf16), struct((feat, count * per_peer), f32), token],
            compiler_params=params(),
            name="sender",
        )(me, node_t, send, edge_t, se_weight, vec)
        if not picks:
            shards = gather_rest(shards, gate)
            send = tie(send, *[shards[m] for m in routed])
            live = jnp.arange(LANES, dtype=jnp.int32)[None, :] < tie(block_count, gate, *[shards[m] for m in [1] + routed])[:, None]
            code = slot_ids.reshape(block_total, LANES) + jnp.where(live, 0, LANES) + 2 * LANES * block_tile[:, None]
            code = lax.all_to_all(code, "peer", 0, 0, tiled=True)
            meta = jnp.concatenate([me, code[:, 0] // (2 * LANES)])
            code = (code & (2 * LANES - 1)).reshape(peers, blocks, LANES)
        picks.append(pick)
        bases.append(base)

    parts = {}
    chain = []
    saved = {}
    got = {}
    both = {}
    for masks in teams:
        count = len(masks)
        extra = len(chain)
        half_at, place = masks[0] % 2, masks[0] // 2
        base = bases[half_at]
        if masks == teams[-1] and len(teams) > 2:
            both = {m: join(parts, got, m) for m in routed if m in parts}
            base = tie(base, *both.values())
        result, act, slope, normed, inv, gate, *pieces = pl.pallas_call(
            functools.partial(forward_kernel, masks, blocks, piece, extra),
            grid_spec=pltpu.PrefetchScalarGridSpec(
                num_scalar_prefetch=1,
                grid=(count, chunks),
                in_specs=[code_of(masks), kept_slab(place), slab_of(masks), whole((feat, feat)), whole((feat, feat)), whole((8, feat, LANES))]
                + [shard_spec] * count
                + [keep_spec] * extra,
                out_specs=[slab_of(masks)] + [own_slab] * 3 + [own_rows, token_spec] + [shard_spec] * count,
                scratch_shapes=[pltpu.VMEM((feat, node_total), f32), pltpu.VMEM((feat, node_total), f32)],
            ),
            out_shape=[slab_shape] + [struct((feat, count * per_peer), bf16)] * 3
            + [struct((count * blocks, LANES), f32), token]
            + [shard_shape] * count,
            input_output_aliases={7 + count: 0} if extra else {},
            compiler_params=params(),
            name="forward",
        )(meta, code, base, edge_t, re_weight, out_t, vec, *[shards[m] for m in masks], *chain)
        chain = [result]
        saved[masks] = (normed, act, slope, inv)
        parts.update(zip(masks, pieces))
        if half_at:
            got.update({m - 1: swap(parts[m], 1) for m in masks})
    edge_result = result
    for m in routed:
        if m not in both:
            both[m] = join(parts, got, m)
    sums = [parts[0], got[0]] + [swap(both[m], m) for m in routed]

    node_result, node_base, back, node_pack = pl.pallas_call(
        functools.partial(node_kernel, len(sums)),
        out_shape=[
            struct((feat, node_total), bf16),
            struct((feat, node_total), f32),
            struct((feat, node_total), bf16),
            struct((feat + 8, 8 * feat), f32),
        ],
        compiler_params=params(),
        name="node",
    )(node_t, node_cot_t, node_in_weight.T, node_back, node_out_t, node_out_weight, vec, *sums)

    backs = gather_first(back)

    parts = {}
    got = {}
    chain = [node_pack]
    first_grads = {}
    for masks in back_teams:
        count = len(masks)
        extra = len(chain)
        half_at, place = masks[0] % 2, masks[0] // 2
        normed, act, slope, inv = saved[masks]
        *outs, = pl.pallas_call(
            functools.partial(backward_kernel, masks, blocks, piece, extra),
            grid_spec=pltpu.PrefetchScalarGridSpec(
                num_scalar_prefetch=1,
                grid=(count, chunks),
                in_specs=[code_of(masks), slab_of(masks)] + [own_slab] * 3 + [own_rows, slab_of(masks), kept_slab(place)]
                + [whole((feat, feat)), whole((feat, feat)), whole((8, feat, LANES))]
                + [shard_spec] * (2 * count)
                + [whole((feat + 8, 8 * feat))]
                + [keep_spec] * (extra - 1),
                out_specs=[slab_of(masks), own_slab, whole((feat + 8, 8 * feat)), token_spec] + [shard_spec] * count,
                scratch_shapes=[
                    pltpu.VMEM((feat, node_total), f32),
                    pltpu.VMEM((feat, node_total), f32),
                    pltpu.VMEM((feat, 2 * feat), f32),
                    pltpu.VMEM((feat, feat), f32),
                    pltpu.VMEM((feat, feat), f32),
                    pltpu.VMEM((4, feat, LANES), f32),
                ],
            ),
            out_shape=[
                struct((feat, edge_total), f32),
                struct((feat, count * per_peer), bf16),
                struct((feat + 8, 8 * feat), f32),
                token,
            ]
            + [shard_shape] * count,
            input_output_aliases={13 + 2 * count: 0} if extra > 1 else {},
            compiler_params=params(),
            name="backward",
        )(
            meta, code, edge_cot_t, normed, act, slope, inv, edge_t, picks[half_at], back_weight, edge_back, vec,
            *[backs[m] for m in masks], *[shards[m] for m in masks], *chain,
        )
        edge_grad, first_grads[masks], edge_pack, gate, *pieces = outs
        chain = [edge_pack, edge_grad]
        parts.update(zip(masks, pieces))
        if half_at:
            got.update({m - 1: swap(parts[m], 1) for m in masks})
        if masks == back_teams[0]:
            backs = gather_rest(backs, gate)

    near_pack = swap(edge_pack, 1)
    late = [m for m in routed if m + 1 in back_teams[-1]]
    early = [m for m in routed if m not in late]
    both = {}
    marks = []
    if early:
        marks = lax.optimization_barrier([got[m] for m in early])
        both = {m: join(parts, {m: value}, m) for m, value in zip(early, marks)}
        marks = [both[m] for m in early]
    there = {m: swap(both[m], m) for m in early}
    edge_pack = edge_pack + tie(near_pack, *marks)
    far = swap(edge_pack, peers // 2) if peers > 2 else None

    sum_wide = min(2048, per_peer)
    sum_chunks = per_peer // sum_wide

    def add_sent(masks_list, hold):
        masks = [m for masks in masks_list for m in masks]
        arrays = [first_grads[masks] for masks in masks_list]
        if hold:
            arrays[0] = tie(arrays[0], *hold)
        spans = [a.shape[1] // sum_wide for a in arrays]
        starts = [sum(spans[:k]) for k in range(len(spans))]

        def send_at(i, ref):
            step = i // sum_chunks
            mask = masks[0]
            for k in range(1, len(masks)):
                mask = jnp.where(step == k, masks[k], mask)
            return ((ref[0] ^ mask) * sum_chunks + i % sum_chunks, 0)

        return pl.pallas_call(
            functools.partial(sender_sum_kernel, tuple(starts)),
            grid_spec=pltpu.PrefetchScalarGridSpec(
                num_scalar_prefetch=1,
                grid=(len(masks) * sum_chunks,),
                in_specs=[pl.BlockSpec((sum_wide // LANES, LANES), send_at)]
                + [
                    pl.BlockSpec((feat, sum_wide), lambda i, ref, start=start, span=span: (0, jnp.clip(i - start, 0, span - 1)))
                    for start, span in zip(starts, spans)
                ],
                out_specs=[shard_spec, token_spec],
                scratch_shapes=[pltpu.VMEM((node_total // WIDE * feat, WIDE), f32), pltpu.VMEM((feat, sum_wide), bf16)],
            ),
            out_shape=[struct((feat, node_total), f32), token],
            compiler_params=params(),
            name="sender_sum",
        )(me, send, *arrays)

    sent_first, gate = add_sent(back_teams[:-1], marks)
    for m in late:
        both[m] = join(parts, {m: tie(got[m], gate)}, m)
        there[m] = swap(both[m], m)
    if far is not None:
        edge_pack = edge_pack + tie(far, gate)
        edge_pack = add_groups(edge_pack)
        mask = 2
        while mask < peers // 2:
            edge_pack = edge_pack + swap(edge_pack, mask)
            mask *= 2
    sent_last, gate = add_sent(back_teams[-1:], [there[m] for m in early])
    sent = [sent_first, sent_last]
    both_packs = tie(edge_pack, gate)
    sums = [parts[0], got[0]] + [there[m] for m in routed]

    vec_out = struct((1, feat), f32)
    node_grad, e1, b1, e2, b2, g1, s1, n1, c1, n2, c2, g2, s2 = pl.pallas_call(
        functools.partial(finish_kernel, len(sent), len(sums)),
        out_shape=[
            struct((feat, node_total), f32),
            struct((feat, 3 * feat), f32), vec_out, struct((feat, feat), f32), vec_out, vec_out, vec_out,
            struct((feat, 2 * feat), f32), vec_out, struct((feat, feat), f32), vec_out, vec_out, vec_out,
        ],
        compiler_params=params(),
        name="finish",
    )(node_base, sr_weight, both_packs, *sent, *sums)

    def flat(row):
        return row.reshape(feat)

    return (
        node_result.T, edge_result.T, node_grad.T, edge_grad.T,
        e1.T, flat(b1), e2, flat(b2), flat(g1), flat(s1),
        n1.T, flat(c1), n2, flat(c2), flat(g2), flat(s2),
    )


def solution(mesh):
    split = P(("grp", "peer"), None)
    line = P(("grp", "peer"))
    one = P()
    return jax.shard_map(
        functools.partial(per_device, mesh.shape["grp"], mesh.shape["peer"]),
        mesh=mesh,
        in_specs=(split, split, line, line, line, line) + (one,) * 12 + (split, split),
        out_specs=(split, split, split, split) + (one,) * 12,
        check_vma=False,
    )
```

```python
import functools

import jax
import jax.numpy as jnp
from jax import lax
from jax.experimental import pallas as pl
from jax.experimental.pallas import tpu as pltpu
from jax.sharding import PartitionSpec as P

epsilon = 1e-05
bf16 = jnp.bfloat16
f32 = jnp.float32
LANES = 128
WIDE = 256


def dot(left, right):
    return jnp.dot(left, right, preferred_element_type=f32)


def dot_nt(left, right):
    return lax.dot_general(left, right, (((1,), (1,)), ((), ())), preferred_element_type=f32)


def dot_exact(left, right):
    return jnp.dot(left, right, preferred_element_type=f32, precision=lax.Precision.HIGHEST)


def dot_nt_exact(left, right):
    return lax.dot_general(
        left,
        right,
        (((1,), (1,)), ((), ())),
        preferred_element_type=f32,
        precision=lax.Precision.HIGHEST,
    )


def params(limit=48):
    return pltpu.CompilerParams(vmem_limit_bytes=limit * 1024 * 1024)


def spread(column, width):
    return jnp.concatenate([column] * (width // LANES), axis=1)


def fold(values):
    total = values[:, :LANES]
    for start in range(LANES, values.shape[1], LANES):
        total = total + values[:, start : start + LANES]
    return total


def row_join(ref, first, count):
    return jnp.concatenate([ref[first + k : first + k + 1, :] for k in range(count)], axis=1)


def sigmoid(values):
    return 0.5 * jnp.tanh(0.5 * values) + 0.5


def onehot_rows(row, rows):
    width = row.shape[1]
    place = lax.broadcasted_iota(jnp.int32, (rows, width), 0)
    return jnp.where(place == row, 1.0, 0.0).astype(bf16)


def onehot_low(row, place):
    spots = jnp.broadcast_to(row.astype(bf16), place.shape)
    return jnp.where(place == spots, jnp.ones((), bf16), jnp.zeros((), bf16))


def place_low():
    return lax.broadcasted_iota(jnp.int32, (LANES, LANES), 0).astype(bf16)


def node_groups(node_ref):
    total = node_ref.shape[1]
    return jnp.concatenate(
        [node_ref[:, start : start + WIDE] for start in range(0, total, WIDE)], axis=0
    )


def sender_kernel(piece, extra, me_ref, node_ref, send_ref, edge_ref, weight_ref, vec_ref, *rest):
    pick_ref, base_ref, token_ref = rest[extra:]
    token_ref[...] = jnp.zeros_like(token_ref)
    width = edge_ref.shape[1]
    feat = edge_ref.shape[0]
    groups = node_ref.shape[1] // WIDE
    table = node_groups(node_ref)
    bias = spread(vec_ref[0], piece)
    place = lax.broadcasted_iota(jnp.int32, (WIDE, piece), 0).astype(bf16)
    for start in range(0, width, piece):
        ids = row_join(send_ref, start // LANES, piece // LANES)
        onehot = onehot_low(ids & (WIDE - 1), place)
        group = lax.shift_right_logical(ids, 8)
        found = dot(table, onehot)
        rows = found[:feat]
        for g in range(1, groups):
            rows = jnp.where(
                jnp.broadcast_to(group == g, (feat, piece)), found[g * feat : (g + 1) * feat], rows
            )
        low = rows.astype(bf16)
        pick_ref[:, start : start + piece] = low
        both = jnp.concatenate([low, edge_ref[:, start : start + piece]], axis=0)
        base_ref[:, start : start + piece] = dot(weight_ref[...], both) + bias


def gather_blocks(meta_ref, first, code_ref, start, count, source_ref):
    feat = source_ref.shape[0]
    parts = []
    for k in range(count):
        tile = meta_ref[first + start + k]
        code = code_ref[0, start + k : start + k + 1, :]
        index = jnp.broadcast_to(code & (LANES - 1), (feat, LANES))
        rows = source_ref[:, pl.ds(pl.multiple_of(tile * LANES, LANES), LANES)]
        taken = jnp.take_along_axis(rows, index, axis=1)
        parts.append(jnp.where(jnp.broadcast_to(code < LANES, (feat, LANES)), taken, 0.0))
    return jnp.concatenate(parts, axis=1)


def scatter_blocks(meta_ref, first, code_ref, start, count, values, total_ref, place):
    for k in range(count):
        tile = meta_ref[first + start + k]
        onehot = onehot_low(code_ref[0, start + k : start + k + 1, :], place)
        term = dot_nt(values[:, k * LANES : (k + 1) * LANES], onehot)
        where_to = pl.ds(pl.multiple_of(tile * LANES, LANES), LANES)
        total_ref[:, where_to] = total_ref[:, where_to] + term


def forward_kernel(masks, blocks, piece, extra, meta_ref, code_ref, base_ref, edge_ref, in_ref, out_ref, vec_ref, *rest):
    count = len(masks)
    shard_refs = rest[:count]
    result_ref, act_ref, slope_ref, normed_ref, inv_ref, token_ref = rest[count + extra : count + extra + 6]
    part_refs = rest[count + extra + 6 : -2]
    proj_ref, total_ref = rest[-2:]
    token_ref[...] = jnp.zeros_like(token_ref)
    step = pl.program_id(0)
    inner = pl.program_id(1)

    @pl.when(inner == 0)
    def _():
        for k in range(count):

            @pl.when(step == k)
            def _():
                proj_ref[...] = dot(in_ref[...], shard_refs[k][...])

        total_ref[...] = jnp.zeros_like(total_ref)

    width = edge_ref.shape[1]
    first = 1 + owner(masks, step, meta_ref) * blocks + inner * (width // LANES)
    per = piece // LANES
    place = place_low()
    for start in range(0, width, piece):
        lanes = slice(start, start + piece)
        block = start // LANES
        half = base_ref[:, lanes] + gather_blocks(meta_ref, first, code_ref, block, per, proj_ref)
        up = jnp.tanh(half) + 1.0
        act = half * up
        slope_ref[:, lanes] = (up + act * (2.0 - up)).astype(bf16)
        act_low = act.astype(bf16)
        act_ref[:, lanes] = act_low
        second = dot(out_ref[...], act_low) + spread(vec_ref[1], piece)
        centered = second - jnp.mean(second, axis=0, keepdims=True)
        inv = lax.rsqrt(jnp.mean(centered * centered, axis=0, keepdims=True) + epsilon)
        normed = centered * inv
        normed_ref[:, lanes] = normed.astype(bf16)
        for k in range(per):
            inv_ref[block + k : block + k + 1, :] = inv[:, k * LANES : (k + 1) * LANES]
        message = (normed * spread(vec_ref[2], piece) + spread(vec_ref[3], piece)).astype(bf16)
        result_ref[:, lanes] = edge_ref[:, lanes] + message
        scatter_blocks(meta_ref, first, code_ref, block, per, message, total_ref, place)

    @pl.when(inner == pl.num_programs(1) - 1)
    def _():
        low = total_ref[...].astype(bf16)
        for k in range(count):

            @pl.when(step == k)
            def _():
                part_refs[k][...] = low


def node_kernel(peers, node_ref, cot_ref, in_t_ref, in_ref, out_t_ref, out_ref, vec_ref, *rest):
    part_refs = rest[:peers]
    result_ref, base_ref, back_ref, pack_ref = rest[peers:]
    feat, total = node_ref.shape
    aggregate = part_refs[0][...].astype(f32)
    for k in range(1, peers):
        aggregate = aggregate + part_refs[k][...].astype(f32)
    node_inputs = jnp.concatenate([node_ref[...], aggregate.astype(bf16)], axis=0)
    pre = dot(in_t_ref[...], node_inputs) + spread(vec_ref[4], total)
    sig = sigmoid(pre)
    act = pre * sig
    slope = sig + act * (1.0 - sig)
    act_low = act.astype(bf16)
    second = dot(out_t_ref[...], act_low) + spread(vec_ref[5], total)
    centered = second - jnp.mean(second, axis=0, keepdims=True)
    inv = lax.rsqrt(jnp.mean(centered * centered, axis=0, keepdims=True) + epsilon)
    normed = centered * inv
    gain = spread(vec_ref[6], total)
    update = normed * gain + spread(vec_ref[7], total)
    result_ref[...] = (node_ref[...].astype(f32) + update).astype(bf16)
    upstream = cot_ref[...].astype(f32)
    scaled = upstream * gain
    inner = (
        scaled
        - jnp.mean(scaled, axis=0, keepdims=True)
        - normed * jnp.mean(scaled * normed, axis=0, keepdims=True)
    )
    grad = (inner * inv).astype(bf16)
    third = (dot(out_ref[...], grad) * slope).astype(bf16)
    input_grad = dot(in_ref[...], third)
    base_ref[...] = upstream + input_grad[:feat]
    back_ref[...] = input_grad[feat:].astype(bf16)
    pack_ref[...] = jnp.zeros_like(pack_ref)
    pack_ref[:feat, 4 * feat : 6 * feat] = dot_nt(third, node_inputs)
    pack_ref[:feat, 6 * feat : 7 * feat] = dot_nt(act_low, grad)
    ones = jnp.ones((8, LANES), f32)
    sums = (
        fold(third.astype(f32)),
        fold(grad.astype(f32)),
        fold(upstream * normed),
        fold(upstream),
    )
    for k in range(4):
        pack_ref[feat + k : feat + k + 1, 4 * feat : 5 * feat] = dot_nt_exact(ones, sums[k])[:1]


def backward_kernel(masks, blocks, piece, extra, meta_ref, code_ref, cot_ref, normed_ref, act_ref, slope_ref, inv_ref, edge_ref, pick_ref, out_ref, in_ref, vec_ref, *rest):
    count = len(masks)
    back_refs = rest[:count]
    shard_refs = rest[count : 2 * count]
    prior_refs = rest[2 * count : 2 * count + extra]
    grad_ref, first_ref, pack_ref, token_ref = rest[2 * count + extra : 2 * count + extra + 4]
    part_refs = rest[2 * count + extra + 4 : -6]
    pull_ref, total_ref, w1_ref, wr_ref, w2_ref, sum_ref = rest[-6:]
    step = pl.program_id(0)
    inner = pl.program_id(1)
    feat, width = edge_ref.shape
    token_ref[...] = jnp.zeros_like(token_ref)

    @pl.when((step == 0) & (inner == 0))
    def _():
        w1_ref[...] = jnp.zeros_like(w1_ref)
        wr_ref[...] = jnp.zeros_like(wr_ref)
        w2_ref[...] = jnp.zeros_like(w2_ref)
        sum_ref[...] = jnp.zeros_like(sum_ref)

    @pl.when(inner == 0)
    def _():
        for k in range(count):

            @pl.when(step == k)
            def _():
                pull_ref[...] = back_refs[k][...].astype(f32)

        total_ref[...] = jnp.zeros_like(total_ref)

    first = 1 + owner(masks, step, meta_ref) * blocks + inner * (width // LANES)
    per = piece // LANES
    place = place_low()
    for start in range(0, width, piece):
        lanes = slice(start, start + piece)
        block = start // LANES
        cot = cot_ref[:, lanes].astype(f32)
        upstream = cot + gather_blocks(meta_ref, first, code_ref, block, per, pull_ref)
        normed = normed_ref[:, lanes].astype(f32)
        scaled = upstream * spread(vec_ref[2], piece)
        inner_grad = (
            scaled
            - jnp.mean(scaled, axis=0, keepdims=True)
            - normed * jnp.mean(scaled * normed, axis=0, keepdims=True)
        )
        second = (inner_grad * row_join(inv_ref, block, per)).astype(bf16)
        sum_ref[2] += fold(upstream * normed)
        sum_ref[3] += fold(upstream)
        sum_ref[1] += fold(second.astype(f32))
        w2_ref[...] += dot_nt(act_ref[:, lanes], second)
        grad = (dot(out_ref[...], second) * slope_ref[:, lanes].astype(f32)).astype(bf16)
        first_ref[:, lanes] = grad
        sum_ref[0] += fold(grad.astype(f32))
        grad_ref[:, lanes] = cot + dot(in_ref[...], grad)
        both = jnp.concatenate([pick_ref[:, lanes], edge_ref[:, lanes]], axis=0)
        w1_ref[...] += dot_nt(grad, both)
        scatter_blocks(meta_ref, first, code_ref, block, per, grad, total_ref, place)
    last = inner == pl.num_programs(1) - 1

    @pl.when(last)
    def _():
        low = total_ref[...].astype(bf16)
        for k in range(count):

            @pl.when(step == k)
            def _():
                part_refs[k][...] = low
                wr_ref[...] += dot_nt(low, shard_refs[k][...])

    @pl.when(last & (step == pl.num_programs(0) - 1))
    def _():
        pack_ref[...] = jnp.zeros_like(pack_ref)
        pack_ref[:feat, :feat] = w1_ref[:, :feat]
        pack_ref[:feat, feat : 2 * feat] = wr_ref[...]
        pack_ref[:feat, 2 * feat : 3 * feat] = w1_ref[:, feat:]
        pack_ref[:feat, 3 * feat : 4 * feat] = w2_ref[...]
        ones = jnp.ones((8, LANES), f32)
        for k in range(4):
            pack_ref[feat + k : feat + k + 1, :feat] = dot_nt_exact(ones, sum_ref[k])[:1]
        pack_ref[...] += prior_refs[0][...]


def sender_sum_kernel(starts, me_ref, send_ref, *rest):
    grad_refs = rest[: len(starts)]
    sum_ref, token_ref, total_ref, grad_ref = rest[len(starts) :]
    feat, width = grad_ref.shape
    groups = sum_ref.shape[1] // WIDE
    step = pl.program_id(0)
    token_ref[...] = jnp.zeros_like(token_ref)
    for k, start in enumerate(starts):
        after = starts[k + 1] if k + 1 < len(starts) else pl.num_programs(0)

        @pl.when((step >= start) & (step < after))
        def _():
            grad_ref[...] = grad_refs[k][...]

    @pl.when(step == 0)
    def _():
        total_ref[...] = jnp.zeros_like(total_ref)

    ids = row_join(send_ref, 0, width // LANES)
    onehot = onehot_rows(ids & (WIDE - 1), WIDE)
    group = jnp.broadcast_to(lax.shift_right_logical(ids, 8).astype(bf16), (feat, width))
    values = grad_ref[...]
    zero = jnp.zeros((), bf16)
    masked = jnp.concatenate(
        [jnp.where(group == jnp.asarray(g, bf16), values, zero) for g in range(groups)], axis=0
    )
    total_ref[...] += dot_nt(masked, onehot)

    @pl.when(step == pl.num_programs(0) - 1)
    def _():
        for g in range(groups):
            sum_ref[:, g * WIDE : (g + 1) * WIDE] = total_ref[g * feat : (g + 1) * feat, :]


def finish_kernel(sums, peers, base_ref, weight_ref, pack_ref, *rest):
    sum_refs = rest[:sums]
    part_refs = rest[sums : sums + peers]
    grad_ref, e1, b1, e2, b2, g1, s1, n1, c1, n2, c2, g2, s2 = rest[sums + peers :]
    sent = sum_refs[0][...]
    for k in range(1, sums):
        sent = sent + sum_refs[k][...]
    total = part_refs[0][...].astype(f32)
    for k in range(1, peers):
        total = total + part_refs[k][...].astype(f32)
    both = jnp.concatenate([sent, total], axis=0)
    grad_ref[...] = base_ref[...] + dot_exact(weight_ref[...], both)
    feat = base_ref.shape[0]
    e1[...] = pack_ref[:feat, : 3 * feat]
    e2[...] = pack_ref[:feat, 3 * feat : 4 * feat]
    n1[...] = pack_ref[:feat, 4 * feat : 6 * feat]
    n2[...] = pack_ref[:feat, 6 * feat : 7 * feat]
    for k, ref in enumerate((b1, b2, g1, s1)):
        ref[...] = pack_ref[feat + k : feat + k + 1, :feat]
    for k, ref in enumerate((c1, c2, g2, s2)):
        ref[...] = pack_ref[feat + k : feat + k + 1, 4 * feat : 5 * feat]


def owner(masks, step, meta_ref):
    stride = masks[1] - masks[0] if len(masks) > 1 else 0
    return meta_ref[0] ^ (masks[0] + stride * step)


def flip(value):
    size = value.shape[1]
    rows = lax.broadcasted_iota(jnp.int32, (size, size), 0)
    cols = lax.broadcasted_iota(jnp.int32, (size, size), 1)
    eye = jnp.where(rows == cols, 1.0, 0.0).astype(bf16)
    return dot_nt(eye, value).astype(value.dtype)


def prepare_kernel(in_ref, out_ref, node_in_ref, node_out_ref, *rest):
    row_refs = rest[:8]
    vec_ref, se_ref, re_ref, out_t_ref, back_ref, edge_back_ref, node_back_ref, node_out_t_ref, sr_ref = rest[8:]
    feat = out_ref.shape[0]
    rows = lax.broadcasted_iota(jnp.int32, (feat, feat), 0)
    cols = lax.broadcasted_iota(jnp.int32, (feat, feat), 1)
    for k in range(8):
        spot = jnp.where(rows == cols, jnp.broadcast_to(row_refs[k][...], (feat, feat)), 0.0)
        column = jnp.sum(spot, axis=1, keepdims=True)
        vec_ref[k] = jnp.broadcast_to(column * 0.5 if k == 0 else column, (feat, LANES))
    half = jnp.asarray(0.5, bf16)
    sent = in_ref[:, :feat]
    received = in_ref[:, feat : 2 * feat]
    edge = in_ref[:, 2 * feat :]
    se_ref[...] = jnp.concatenate([sent, edge], axis=1) * half
    re_ref[...] = received * half
    out_t_ref[...] = flip(out_ref[...])
    back_ref[...] = out_ref[...] * half
    edge_back_ref[...] = flip(edge)
    node_back_ref[:feat] = flip(node_in_ref[:, :feat])
    node_back_ref[feat:] = flip(node_in_ref[:, feat:])
    node_out_t_ref[...] = flip(node_out_ref[...])
    sr_ref[...] = jnp.concatenate([flip(sent), flip(received)], axis=1).astype(f32)


def struct(shape, dtype):
    return jax.ShapeDtypeStruct(shape, dtype)


def whole(shape):
    return pl.BlockSpec(shape, lambda *_: (0,) * len(shape))


def per_device(groups, peers, *arrays):
    (
        nodes, edges, send_nodes, block_tile, block_count, slot_ids,
        edge_in_weight, edge_in_bias, edge_out_weight, edge_out_bias, edge_gain, edge_shift,
        node_in_weight, node_in_bias, node_out_weight, node_out_bias, node_gain, node_shift,
        node_cot, edge_cot,
    ) = arrays
    feat = nodes.shape[1]
    node_total = nodes.shape[0]
    edge_total = edges.shape[0]
    block_total = block_tile.shape[0]
    blocks = block_total // peers
    per_peer = edge_total // peers
    rows = edge_total // LANES

    def swap(value, mask):
        if mask == 0:
            return value
        return lax.ppermute(value, "peer", [(i, i ^ mask) for i in range(peers)])

    near = [m for m in range(0, peers, 2)]
    routed = [m for m in (4, 6, 2) if m < peers] + [m for m in range(8, peers, 2)]

    def tie(value, *others):
        return lax.optimization_barrier((value,) + others)[0]

    def gather_first(value):
        return {m: swap(value, m) for m in [0, 1] + routed}

    def gather_rest(found, gate):
        for m in routed:
            found[m | 1] = swap(tie(found[m], gate), 1)
        return found

    def join(parts, got, m):
        return (parts[m].astype(f32) + got[m].astype(f32)).astype(bf16)

    def add_groups(value):
        if groups > 4:
            mask = 1
            while mask < groups:
                value = value + lax.ppermute(value, "grp", [(i, i ^ mask) for i in range(groups)])
                mask *= 2
            return value
        others = [lax.ppermute(value, "grp", [(i, i ^ mask) for i in range(groups)]) for mask in range(1, groups)]
        return sum(others, value)

    halves = [tuple(range(0, peers, 2)), tuple(range(1, peers, 2))]
    firsts_of = list(range(0, peers, 4))
    pair = lambda m: (m, m + 2) if m + 2 < peers else (m,)
    teams = [pair(m + side) for m in firsts_of[::-1] for side in (1, 0)]
    back_teams = [pair(0)]
    for m in firsts_of[1:]:
        back_teams += [pair(m), pair(m + 1)]
    back_teams.append(pair(1))

    node_t = nodes.T
    edge_t = edges.T
    node_cot_t = node_cot.T
    edge_cot_t = edge_cot.T
    in_t = edge_in_weight.T
    send = send_nodes.reshape(rows, LANES)
    me = lax.axis_index("peer").astype(jnp.int32)[None]

    shards = gather_first(node_t)

    square = struct((feat, feat), bf16)
    vec, se_weight, re_weight, out_t, back_weight, edge_back, node_back, node_out_t, sr_weight = pl.pallas_call(
        prepare_kernel,
        out_shape=[
            struct((8, feat, LANES), f32), struct((feat, 2 * feat), bf16), square, square, square, square,
            struct((2 * feat, feat), bf16), square, struct((feat, 2 * feat), f32),
        ],
        name="prepare",
    )(
        in_t, edge_out_weight, node_in_weight.T, node_out_weight,
        *[v[None] for v in (edge_in_bias, edge_out_bias, edge_gain, edge_shift, node_in_bias, node_out_bias, node_gain, node_shift)],
    )

    wide = min(4096, per_peer)
    chunks = per_peer // wide
    sub = wide // LANES
    piece = min(2048, wide)

    def slab_of(masks):
        return pl.BlockSpec((feat, wide), lambda i, j, ref: (0, owner(masks, i, ref) * chunks + j))

    def rows_of(masks):
        return pl.BlockSpec((sub, LANES), lambda i, j, ref: (owner(masks, i, ref) * chunks + j, 0))

    def code_of(masks):
        return pl.BlockSpec((1, sub, LANES), lambda i, j, ref: (owner(masks, i, ref), j, 0))

    def kept_slab(place):
        return pl.BlockSpec((feat, wide), lambda i, j, ref: (0, (place + i) * chunks + j))

    own_slab = kept_slab(0)
    own_rows = pl.BlockSpec((sub, LANES), lambda i, j, ref: (i * chunks + j, 0))
    shard_spec = whole((feat, node_total))
    keep_spec = pl.BlockSpec(memory_space=pl.ANY)

    token = struct((8, LANES), f32)
    token_spec = whole((8, LANES))
    slab_shape = struct((feat, edge_total), bf16)
    shard_shape = struct((feat, node_total), bf16)
    picks, bases = [], []
    for masks in halves:
        count = len(masks)
        pick, base, gate = pl.pallas_call(
            functools.partial(sender_kernel, min(2048, wide), 0),
            grid_spec=pltpu.PrefetchScalarGridSpec(
                num_scalar_prefetch=1,
                grid=(count, chunks),
                in_specs=[shard_spec, rows_of(masks), slab_of(masks), whole((feat, 2 * feat)), whole((8, feat, LANES))],
                out_specs=[own_slab, own_slab, token_spec],
            ),
            out_shape=[struct((feat, count * per_peer), bf16), struct((feat, count * per_peer), f32), token],
            compiler_params=params(),
            name="sender",
        )(me, node_t, send, edge_t, se_weight, vec)
        if not picks:
            shards = gather_rest(shards, gate)
            send = tie(send, *[shards[m] for m in routed])
            live = jnp.arange(LANES, dtype=jnp.int32)[None, :] < tie(block_count, gate, *[shards[m] for m in [1] + routed])[:, None]
            code = slot_ids.reshape(block_total, LANES) + jnp.where(live, 0, LANES) + 2 * LANES * block_tile[:, None]
            code = lax.all_to_all(code, "peer", 0, 0, tiled=True)
            meta = jnp.concatenate([me, code[:, 0] // (2 * LANES)])
            code = (code & (2 * LANES - 1)).reshape(peers, blocks, LANES)
        picks.append(pick)
        bases.append(base)

    parts = {}
    chain = []
    saved = {}
    got = {}
    both = {}
    for masks in teams:
        count = len(masks)
        extra = len(chain)
        half_at, place = masks[0] % 2, masks[0] // 2
        base = bases[half_at]
        if masks == teams[-1] and len(teams) > 2:
            both = {m: join(parts, got, m) for m in routed if m in parts}
            base = tie(base, *both.values())
        result, act, slope, normed, inv, gate, *pieces = pl.pallas_call(
            functools.partial(forward_kernel, masks, blocks, piece, extra),
            grid_spec=pltpu.PrefetchScalarGridSpec(
                num_scalar_prefetch=1,
                grid=(count, chunks),
                in_specs=[code_of(masks), kept_slab(place), slab_of(masks), whole((feat, feat)), whole((feat, feat)), whole((8, feat, LANES))]
                + [shard_spec] * count
                + [keep_spec] * extra,
                out_specs=[slab_of(masks)] + [own_slab] * 3 + [own_rows, token_spec] + [shard_spec] * count,
                scratch_shapes=[pltpu.VMEM((feat, node_total), f32), pltpu.VMEM((feat, node_total), f32)],
            ),
            out_shape=[slab_shape] + [struct((feat, count * per_peer), bf16)] * 3
            + [struct((count * blocks, LANES), f32), token]
            + [shard_shape] * count,
            input_output_aliases={7 + count: 0} if extra else {},
            compiler_params=params(),
            name="forward",
        )(meta, code, base, edge_t, re_weight, out_t, vec, *[shards[m] for m in masks], *chain)
        chain = [result]
        saved[masks] = (normed, act, slope, inv)
        parts.update(zip(masks, pieces))
        if half_at:
            got.update({m - 1: swap(parts[m], 1) for m in masks})
    edge_result = result
    for m in routed:
        if m not in both:
            both[m] = join(parts, got, m)
    sums = [parts[0], got[0]] + [swap(both[m], m) for m in routed]

    node_result, node_base, back, node_pack = pl.pallas_call(
        functools.partial(node_kernel, len(sums)),
        out_shape=[
            struct((feat, node_total), bf16),
            struct((feat, node_total), f32),
            struct((feat, node_total), bf16),
            struct((feat + 8, 8 * feat), f32),
        ],
        compiler_params=params(),
        name="node",
    )(node_t, node_cot_t, node_in_weight.T, node_back, node_out_t, node_out_weight, vec, *sums)

    backs = gather_first(back)

    parts = {}
    got = {}
    chain = [node_pack]
    first_grads = {}
    for masks in back_teams:
        count = len(masks)
        extra = len(chain)
        half_at, place = masks[0] % 2, masks[0] // 2
        normed, act, slope, inv = saved[masks]
        *outs, = pl.pallas_call(
            functools.partial(backward_kernel, masks, blocks, piece, extra),
            grid_spec=pltpu.PrefetchScalarGridSpec(
                num_scalar_prefetch=1,
                grid=(count, chunks),
                in_specs=[code_of(masks), slab_of(masks)] + [own_slab] * 3 + [own_rows, slab_of(masks), kept_slab(place)]
                + [whole((feat, feat)), whole((feat, feat)), whole((8, feat, LANES))]
                + [shard_spec] * (2 * count)
                + [whole((feat + 8, 8 * feat))]
                + [keep_spec] * (extra - 1),
                out_specs=[slab_of(masks), own_slab, whole((feat + 8, 8 * feat)), token_spec] + [shard_spec] * count,
                scratch_shapes=[
                    pltpu.VMEM((feat, node_total), f32),
                    pltpu.VMEM((feat, node_total), f32),
                    pltpu.VMEM((feat, 2 * feat), f32),
                    pltpu.VMEM((feat, feat), f32),
                    pltpu.VMEM((feat, feat), f32),
                    pltpu.VMEM((4, feat, LANES), f32),
                ],
            ),
            out_shape=[
                struct((feat, edge_total), f32),
                struct((feat, count * per_peer), bf16),
                struct((feat + 8, 8 * feat), f32),
                token,
            ]
            + [shard_shape] * count,
            input_output_aliases={13 + 2 * count: 0} if extra > 1 else {},
            compiler_params=params(),
            name="backward",
        )(
            meta, code, edge_cot_t, normed, act, slope, inv, edge_t, picks[half_at], back_weight, edge_back, vec,
            *[backs[m] for m in masks], *[shards[m] for m in masks], *chain,
        )
        edge_grad, first_grads[masks], edge_pack, gate, *pieces = outs
        chain = [edge_pack, edge_grad]
        parts.update(zip(masks, pieces))
        if half_at:
            got.update({m - 1: swap(parts[m], 1) for m in masks})
        if masks == back_teams[0]:
            backs = gather_rest(backs, gate)

    near_pack = swap(edge_pack, 1)
    late = [m for m in routed if m + 1 in back_teams[-1]]
    early = [m for m in routed if m not in late]
    both = {}
    marks = []
    if early:
        marks = lax.optimization_barrier([got[m] for m in early])
        both = {m: join(parts, {m: value}, m) for m, value in zip(early, marks)}
        marks = [both[m] for m in early]
    there = {m: swap(both[m], m) for m in early}
    edge_pack = edge_pack + tie(near_pack, *marks)
    far = swap(edge_pack, peers // 2) if peers > 2 else None

    sum_wide = min(2048, per_peer)
    sum_chunks = per_peer // sum_wide

    def add_sent(masks_list, hold):
        masks = [m for masks in masks_list for m in masks]
        arrays = [first_grads[masks] for masks in masks_list]
        if hold:
            arrays[0] = tie(arrays[0], *hold)
        spans = [a.shape[1] // sum_wide for a in arrays]
        starts = [sum(spans[:k]) for k in range(len(spans))]

        def send_at(i, ref):
            step = i // sum_chunks
            mask = masks[0]
            for k in range(1, len(masks)):
                mask = jnp.where(step == k, masks[k], mask)
            return ((ref[0] ^ mask) * sum_chunks + i % sum_chunks, 0)

        return pl.pallas_call(
            functools.partial(sender_sum_kernel, tuple(starts)),
            grid_spec=pltpu.PrefetchScalarGridSpec(
                num_scalar_prefetch=1,
                grid=(len(masks) * sum_chunks,),
                in_specs=[pl.BlockSpec((sum_wide // LANES, LANES), send_at)]
                + [
                    pl.BlockSpec((feat, sum_wide), lambda i, ref, start=start, span=span: (0, jnp.clip(i - start, 0, span - 1)))
                    for start, span in zip(starts, spans)
                ],
                out_specs=[shard_spec, token_spec],
                scratch_shapes=[pltpu.VMEM((node_total // WIDE * feat, WIDE), f32), pltpu.VMEM((feat, sum_wide), bf16)],
            ),
            out_shape=[struct((feat, node_total), f32), token],
            compiler_params=params(),
            name="sender_sum",
        )(me, send, *arrays)

    sent_first, gate = add_sent(back_teams[:-1], marks)
    for m in late:
        both[m] = join(parts, {m: tie(got[m], gate)}, m)
        there[m] = swap(both[m], m)
    if far is not None:
        edge_pack = edge_pack + tie(far, gate)
        edge_pack = add_groups(tie(edge_pack, got[0]))
        mask = 2
        while mask < peers // 2:
            edge_pack = edge_pack + swap(edge_pack, mask)
            mask *= 2
    sent_last, gate = add_sent(back_teams[-1:], [there[m] for m in early])
    sent = [sent_first, sent_last]
    both_packs = tie(edge_pack, gate)
    sums = [parts[0], got[0]] + [there[m] for m in routed]

    vec_out = struct((1, feat), f32)
    node_grad, e1, b1, e2, b2, g1, s1, n1, c1, n2, c2, g2, s2 = pl.pallas_call(
        functools.partial(finish_kernel, len(sent), len(sums)),
        out_shape=[
            struct((feat, node_total), f32),
            struct((feat, 3 * feat), f32), vec_out, struct((feat, feat), f32), vec_out, vec_out, vec_out,
            struct((feat, 2 * feat), f32), vec_out, struct((feat, feat), f32), vec_out, vec_out, vec_out,
        ],
        compiler_params=params(),
        name="finish",
    )(node_base, sr_weight, both_packs, *sent, *sums)

    def flat(row):
        return row.reshape(feat)

    return (
        node_result.T, edge_result.T, node_grad.T, edge_grad.T,
        e1.T, flat(b1), e2, flat(b2), flat(g1), flat(s1),
        n1.T, flat(c1), n2, flat(c2), flat(g2), flat(s2),
    )


def solution(mesh):
    split = P(("grp", "peer"), None)
    line = P(("grp", "peer"))
    one = P()
    return jax.shard_map(
        functools.partial(per_device, mesh.shape["grp"], mesh.shape["peer"]),
        mesh=mesh,
        in_specs=(split, split, line, line, line, line) + (one,) * 12 + (split, split),
        out_specs=(split, split, split, split) + (one,) * 12,
        check_vma=False,
    )
```

```python
import functools

import jax
import jax.numpy as jnp
from jax import lax
from jax.experimental import pallas as pl
from jax.experimental.pallas import tpu as pltpu
from jax.sharding import PartitionSpec as P

epsilon = 1e-05
bf16 = jnp.bfloat16
f32 = jnp.float32
LANES = 128
WIDE = 256


def dot(left, right):
    return jnp.dot(left, right, preferred_element_type=f32)


def dot_nt(left, right):
    return lax.dot_general(left, right, (((1,), (1,)), ((), ())), preferred_element_type=f32)


def dot_exact(left, right):
    return jnp.dot(left, right, preferred_element_type=f32, precision=lax.Precision.HIGHEST)


def dot_nt_exact(left, right):
    return lax.dot_general(
        left,
        right,
        (((1,), (1,)), ((), ())),
        preferred_element_type=f32,
        precision=lax.Precision.HIGHEST,
    )


def params(limit=48):
    return pltpu.CompilerParams(vmem_limit_bytes=limit * 1024 * 1024)


def spread(column, width):
    return jnp.concatenate([column] * (width // LANES), axis=1)


def fold(values):
    total = values[:, :LANES]
    for start in range(LANES, values.shape[1], LANES):
        total = total + values[:, start : start + LANES]
    return total


def row_join(ref, first, count):
    return jnp.concatenate([ref[first + k : first + k + 1, :] for k in range(count)], axis=1)


def sigmoid(values):
    return 0.5 * jnp.tanh(0.5 * values) + 0.5


def onehot_rows(row, rows):
    width = row.shape[1]
    place = lax.broadcasted_iota(jnp.int32, (rows, width), 0)
    return jnp.where(place == row, 1.0, 0.0).astype(bf16)


def onehot_low(row, place):
    spots = jnp.broadcast_to(row.astype(bf16), place.shape)
    return jnp.where(place == spots, jnp.ones((), bf16), jnp.zeros((), bf16))


def place_low():
    return lax.broadcasted_iota(jnp.int32, (LANES, LANES), 0).astype(bf16)


def node_groups(node_ref):
    total = node_ref.shape[1]
    return jnp.concatenate(
        [node_ref[:, start : start + WIDE] for start in range(0, total, WIDE)], axis=0
    )


def sender_kernel(piece, extra, me_ref, node_ref, send_ref, edge_ref, weight_ref, vec_ref, *rest):
    pick_ref, base_ref, token_ref = rest[extra:]
    token_ref[...] = jnp.zeros_like(token_ref)
    width = edge_ref.shape[1]
    feat = edge_ref.shape[0]
    groups = node_ref.shape[1] // WIDE
    table = node_groups(node_ref)
    bias = spread(vec_ref[0], piece)
    place = lax.broadcasted_iota(jnp.int32, (WIDE, piece), 0).astype(bf16)
    for start in range(0, width, piece):
        ids = row_join(send_ref, start // LANES, piece // LANES)
        onehot = onehot_low(ids & (WIDE - 1), place)
        group = lax.shift_right_logical(ids, 8)
        found = dot(table, onehot)
        rows = found[:feat]
        for g in range(1, groups):
            rows = jnp.where(
                jnp.broadcast_to(group == g, (feat, piece)), found[g * feat : (g + 1) * feat], rows
            )
        low = rows.astype(bf16)
        pick_ref[:, start : start + piece] = low
        both = jnp.concatenate([low, edge_ref[:, start : start + piece]], axis=0)
        base_ref[:, start : start + piece] = dot(weight_ref[...], both) + bias


def gather_blocks(meta_ref, first, code_ref, start, count, source_ref):
    feat = source_ref.shape[0]
    parts = []
    for k in range(count):
        tile = meta_ref[first + start + k]
        code = code_ref[0, start + k : start + k + 1, :]
        index = jnp.broadcast_to(code & (LANES - 1), (feat, LANES))
        rows = source_ref[:, pl.ds(pl.multiple_of(tile * LANES, LANES), LANES)]
        taken = jnp.take_along_axis(rows, index, axis=1)
        parts.append(jnp.where(jnp.broadcast_to(code < LANES, (feat, LANES)), taken, 0.0))
    return jnp.concatenate(parts, axis=1)


def scatter_blocks(meta_ref, first, code_ref, start, count, values, total_ref, place):
    for k in range(count):
        tile = meta_ref[first + start + k]
        onehot = onehot_low(code_ref[0, start + k : start + k + 1, :], place)
        term = dot_nt(values[:, k * LANES : (k + 1) * LANES], onehot)
        where_to = pl.ds(pl.multiple_of(tile * LANES, LANES), LANES)
        total_ref[:, where_to] = total_ref[:, where_to] + term


def forward_kernel(masks, blocks, piece, extra, meta_ref, code_ref, base_ref, edge_ref, in_ref, out_ref, vec_ref, *rest):
    count = len(masks)
    shard_refs = rest[:count]
    result_ref, act_ref, slope_ref, normed_ref, inv_ref, token_ref = rest[count + extra : count + extra + 6]
    part_refs = rest[count + extra + 6 : -2]
    proj_ref, total_ref = rest[-2:]
    token_ref[...] = jnp.zeros_like(token_ref)
    step = pl.program_id(0)
    inner = pl.program_id(1)

    @pl.when(inner == 0)
    def _():
        for k in range(count):

            @pl.when(step == k)
            def _():
                proj_ref[...] = dot(in_ref[...], shard_refs[k][...])

        total_ref[...] = jnp.zeros_like(total_ref)

    width = edge_ref.shape[1]
    first = 1 + owner(masks, step, meta_ref) * blocks + inner * (width // LANES)
    per = piece // LANES
    place = place_low()
    for start in range(0, width, piece):
        lanes = slice(start, start + piece)
        block = start // LANES
        half = base_ref[:, lanes] + gather_blocks(meta_ref, first, code_ref, block, per, proj_ref)
        up = jnp.tanh(half) + 1.0
        act = half * up
        slope_ref[:, lanes] = (up + act * (2.0 - up)).astype(bf16)
        act_low = act.astype(bf16)
        act_ref[:, lanes] = act_low
        second = dot(out_ref[...], act_low) + spread(vec_ref[1], piece)
        centered = second - jnp.mean(second, axis=0, keepdims=True)
        inv = lax.rsqrt(jnp.mean(centered * centered, axis=0, keepdims=True) + epsilon)
        normed = centered * inv
        normed_ref[:, lanes] = normed.astype(bf16)
        for k in range(per):
            inv_ref[block + k : block + k + 1, :] = inv[:, k * LANES : (k + 1) * LANES]
        message = (normed * spread(vec_ref[2], piece) + spread(vec_ref[3], piece)).astype(bf16)
        result_ref[:, lanes] = edge_ref[:, lanes] + message
        scatter_blocks(meta_ref, first, code_ref, block, per, message, total_ref, place)

    @pl.when(inner == pl.num_programs(1) - 1)
    def _():
        low = total_ref[...].astype(bf16)
        for k in range(count):

            @pl.when(step == k)
            def _():
                part_refs[k][...] = low


def node_kernel(peers, node_ref, cot_ref, in_t_ref, in_ref, out_t_ref, out_ref, vec_ref, *rest):
    part_refs = rest[:peers]
    result_ref, base_ref, back_ref, pack_ref = rest[peers:]
    feat, total = node_ref.shape
    aggregate = part_refs[0][...].astype(f32)
    for k in range(1, peers):
        aggregate = aggregate + part_refs[k][...].astype(f32)
    node_inputs = jnp.concatenate([node_ref[...], aggregate.astype(bf16)], axis=0)
    pre = dot(in_t_ref[...], node_inputs) + spread(vec_ref[4], total)
    sig = sigmoid(pre)
    act = pre * sig
    slope = sig + act * (1.0 - sig)
    act_low = act.astype(bf16)
    second = dot(out_t_ref[...], act_low) + spread(vec_ref[5], total)
    centered = second - jnp.mean(second, axis=0, keepdims=True)
    inv = lax.rsqrt(jnp.mean(centered * centered, axis=0, keepdims=True) + epsilon)
    normed = centered * inv
    gain = spread(vec_ref[6], total)
    update = normed * gain + spread(vec_ref[7], total)
    result_ref[...] = (node_ref[...].astype(f32) + update).astype(bf16)
    upstream = cot_ref[...].astype(f32)
    scaled = upstream * gain
    inner = (
        scaled
        - jnp.mean(scaled, axis=0, keepdims=True)
        - normed * jnp.mean(scaled * normed, axis=0, keepdims=True)
    )
    grad = (inner * inv).astype(bf16)
    third = (dot(out_ref[...], grad) * slope).astype(bf16)
    input_grad = dot(in_ref[...], third)
    base_ref[...] = upstream + input_grad[:feat]
    back_ref[...] = input_grad[feat:].astype(bf16)
    pack_ref[...] = jnp.zeros_like(pack_ref)
    pack_ref[:feat, 4 * feat : 6 * feat] = dot_nt(third, node_inputs)
    pack_ref[:feat, 6 * feat : 7 * feat] = dot_nt(act_low, grad)
    ones = jnp.ones((8, LANES), f32)
    sums = (
        fold(third.astype(f32)),
        fold(grad.astype(f32)),
        fold(upstream * normed),
        fold(upstream),
    )
    for k in range(4):
        pack_ref[feat + k : feat + k + 1, 4 * feat : 5 * feat] = dot_nt_exact(ones, sums[k])[:1]


def backward_kernel(masks, blocks, piece, extra, meta_ref, code_ref, cot_ref, normed_ref, act_ref, slope_ref, inv_ref, edge_ref, pick_ref, out_ref, in_ref, vec_ref, *rest):
    count = len(masks)
    back_refs = rest[:count]
    shard_refs = rest[count : 2 * count]
    prior_refs = rest[2 * count : 2 * count + extra]
    grad_ref, first_ref, pack_ref, token_ref = rest[2 * count + extra : 2 * count + extra + 4]
    part_refs = rest[2 * count + extra + 4 : -6]
    pull_ref, total_ref, w1_ref, wr_ref, w2_ref, sum_ref = rest[-6:]
    step = pl.program_id(0)
    inner = pl.program_id(1)
    feat, width = edge_ref.shape
    token_ref[...] = jnp.zeros_like(token_ref)

    @pl.when((step == 0) & (inner == 0))
    def _():
        w1_ref[...] = jnp.zeros_like(w1_ref)
        wr_ref[...] = jnp.zeros_like(wr_ref)
        w2_ref[...] = jnp.zeros_like(w2_ref)
        sum_ref[...] = jnp.zeros_like(sum_ref)

    @pl.when(inner == 0)
    def _():
        for k in range(count):

            @pl.when(step == k)
            def _():
                pull_ref[...] = back_refs[k][...].astype(f32)

        total_ref[...] = jnp.zeros_like(total_ref)

    first = 1 + owner(masks, step, meta_ref) * blocks + inner * (width // LANES)
    per = piece // LANES
    place = place_low()
    for start in range(0, width, piece):
        lanes = slice(start, start + piece)
        block = start // LANES
        cot = cot_ref[:, lanes].astype(f32)
        upstream = cot + gather_blocks(meta_ref, first, code_ref, block, per, pull_ref)
        normed = normed_ref[:, lanes].astype(f32)
        scaled = upstream * spread(vec_ref[2], piece)
        inner_grad = (
            scaled
            - jnp.mean(scaled, axis=0, keepdims=True)
            - normed * jnp.mean(scaled * normed, axis=0, keepdims=True)
        )
        second = (inner_grad * row_join(inv_ref, block, per)).astype(bf16)
        sum_ref[2] += fold(upstream * normed)
        sum_ref[3] += fold(upstream)
        sum_ref[1] += fold(second.astype(f32))
        w2_ref[...] += dot_nt(act_ref[:, lanes], second)
        grad = (dot(out_ref[...], second) * slope_ref[:, lanes].astype(f32)).astype(bf16)
        first_ref[:, lanes] = grad
        sum_ref[0] += fold(grad.astype(f32))
        grad_ref[:, lanes] = cot + dot(in_ref[...], grad)
        both = jnp.concatenate([pick_ref[:, lanes], edge_ref[:, lanes]], axis=0)
        w1_ref[...] += dot_nt(grad, both)
        scatter_blocks(meta_ref, first, code_ref, block, per, grad, total_ref, place)
    last = inner == pl.num_programs(1) - 1

    @pl.when(last)
    def _():
        low = total_ref[...].astype(bf16)
        for k in range(count):

            @pl.when(step == k)
            def _():
                part_refs[k][...] = low
                wr_ref[...] += dot_nt(low, shard_refs[k][...])

    @pl.when(last & (step == pl.num_programs(0) - 1))
    def _():
        pack_ref[...] = jnp.zeros_like(pack_ref)
        pack_ref[:feat, :feat] = w1_ref[:, :feat]
        pack_ref[:feat, feat : 2 * feat] = wr_ref[...]
        pack_ref[:feat, 2 * feat : 3 * feat] = w1_ref[:, feat:]
        pack_ref[:feat, 3 * feat : 4 * feat] = w2_ref[...]
        ones = jnp.ones((8, LANES), f32)
        for k in range(4):
            pack_ref[feat + k : feat + k + 1, :feat] = dot_nt_exact(ones, sum_ref[k])[:1]
        pack_ref[...] += prior_refs[0][...]


def sender_sum_kernel(starts, me_ref, send_ref, *rest):
    grad_refs = rest[: len(starts)]
    sum_ref, token_ref, total_ref, grad_ref = rest[len(starts) :]
    feat, width = grad_ref.shape
    groups = sum_ref.shape[1] // WIDE
    step = pl.program_id(0)
    token_ref[...] = jnp.zeros_like(token_ref)
    for k, start in enumerate(starts):
        after = starts[k + 1] if k + 1 < len(starts) else pl.num_programs(0)

        @pl.when((step >= start) & (step < after))
        def _():
            grad_ref[...] = grad_refs[k][...]

    @pl.when(step == 0)
    def _():
        total_ref[...] = jnp.zeros_like(total_ref)

    ids = row_join(send_ref, 0, width // LANES)
    onehot = onehot_rows(ids & (WIDE - 1), WIDE)
    group = jnp.broadcast_to(lax.shift_right_logical(ids, 8).astype(bf16), (feat, width))
    values = grad_ref[...]
    zero = jnp.zeros((), bf16)
    masked = jnp.concatenate(
        [jnp.where(group == jnp.asarray(g, bf16), values, zero) for g in range(groups)], axis=0
    )
    total_ref[...] += dot_nt(masked, onehot)

    @pl.when(step == pl.num_programs(0) - 1)
    def _():
        for g in range(groups):
            sum_ref[:, g * WIDE : (g + 1) * WIDE] = total_ref[g * feat : (g + 1) * feat, :]


def finish_kernel(sums, peers, base_ref, weight_ref, pack_ref, *rest):
    sum_refs = rest[:sums]
    part_refs = rest[sums : sums + peers]
    grad_ref, e1, b1, e2, b2, g1, s1, n1, c1, n2, c2, g2, s2 = rest[sums + peers :]
    sent = sum_refs[0][...]
    for k in range(1, sums):
        sent = sent + sum_refs[k][...]
    total = part_refs[0][...].astype(f32)
    for k in range(1, peers):
        total = total + part_refs[k][...].astype(f32)
    both = jnp.concatenate([sent, total], axis=0)
    grad_ref[...] = base_ref[...] + dot_exact(weight_ref[...], both)
    feat = base_ref.shape[0]
    e1[...] = pack_ref[:feat, : 3 * feat]
    e2[...] = pack_ref[:feat, 3 * feat : 4 * feat]
    n1[...] = pack_ref[:feat, 4 * feat : 6 * feat]
    n2[...] = pack_ref[:feat, 6 * feat : 7 * feat]
    for k, ref in enumerate((b1, b2, g1, s1)):
        ref[...] = pack_ref[feat + k : feat + k + 1, :feat]
    for k, ref in enumerate((c1, c2, g2, s2)):
        ref[...] = pack_ref[feat + k : feat + k + 1, 4 * feat : 5 * feat]


def owner(masks, step, meta_ref):
    stride = masks[1] - masks[0] if len(masks) > 1 else 0
    return meta_ref[0] ^ (masks[0] + stride * step)


def flip(value):
    size = value.shape[1]
    rows = lax.broadcasted_iota(jnp.int32, (size, size), 0)
    cols = lax.broadcasted_iota(jnp.int32, (size, size), 1)
    eye = jnp.where(rows == cols, 1.0, 0.0).astype(bf16)
    return dot_nt(eye, value).astype(value.dtype)


def prepare_kernel(in_ref, out_ref, node_in_ref, node_out_ref, *rest):
    row_refs = rest[:8]
    vec_ref, se_ref, re_ref, out_t_ref, back_ref, edge_back_ref, node_back_ref, node_out_t_ref, sr_ref = rest[8:]
    feat = out_ref.shape[0]
    rows = lax.broadcasted_iota(jnp.int32, (feat, feat), 0)
    cols = lax.broadcasted_iota(jnp.int32, (feat, feat), 1)
    for k in range(8):
        spot = jnp.where(rows == cols, jnp.broadcast_to(row_refs[k][...], (feat, feat)), 0.0)
        column = jnp.sum(spot, axis=1, keepdims=True)
        vec_ref[k] = jnp.broadcast_to(column * 0.5 if k == 0 else column, (feat, LANES))
    half = jnp.asarray(0.5, bf16)
    sent = in_ref[:, :feat]
    received = in_ref[:, feat : 2 * feat]
    edge = in_ref[:, 2 * feat :]
    se_ref[...] = jnp.concatenate([sent, edge], axis=1) * half
    re_ref[...] = received * half
    out_t_ref[...] = flip(out_ref[...])
    back_ref[...] = out_ref[...] * half
    edge_back_ref[...] = flip(edge)
    node_back_ref[:feat] = flip(node_in_ref[:, :feat])
    node_back_ref[feat:] = flip(node_in_ref[:, feat:])
    node_out_t_ref[...] = flip(node_out_ref[...])
    sr_ref[...] = jnp.concatenate([flip(sent), flip(received)], axis=1).astype(f32)


def struct(shape, dtype):
    return jax.ShapeDtypeStruct(shape, dtype)


def whole(shape):
    return pl.BlockSpec(shape, lambda *_: (0,) * len(shape))


def per_device(groups, peers, *arrays):
    (
        nodes, edges, send_nodes, block_tile, block_count, slot_ids,
        edge_in_weight, edge_in_bias, edge_out_weight, edge_out_bias, edge_gain, edge_shift,
        node_in_weight, node_in_bias, node_out_weight, node_out_bias, node_gain, node_shift,
        node_cot, edge_cot,
    ) = arrays
    feat = nodes.shape[1]
    node_total = nodes.shape[0]
    edge_total = edges.shape[0]
    block_total = block_tile.shape[0]
    blocks = block_total // peers
    per_peer = edge_total // peers
    rows = edge_total // LANES

    def swap(value, mask):
        if mask == 0:
            return value
        return lax.ppermute(value, "peer", [(i, i ^ mask) for i in range(peers)])

    near = [m for m in range(0, peers, 2)]
    routed = [m for m in (4, 6, 2) if m < peers] + [m for m in range(8, peers, 2)]

    def tie(value, *others):
        return lax.optimization_barrier((value,) + others)[0]

    def gather_first(value):
        return {m: swap(value, m) for m in [0] + routed + [1]}

    def gather_rest(found, gate):
        for m in routed:
            found[m | 1] = swap(tie(found[m], gate), 1)
        return found

    def join(parts, got, m):
        return (parts[m].astype(f32) + got[m].astype(f32)).astype(bf16)

    def add_groups(value):
        if groups > 4:
            mask = 1
            while mask < groups:
                value = value + lax.ppermute(value, "grp", [(i, i ^ mask) for i in range(groups)])
                mask *= 2
            return value
        others = [lax.ppermute(value, "grp", [(i, i ^ mask) for i in range(groups)]) for mask in range(1, groups)]
        return sum(others, value)

    halves = [tuple(range(0, peers, 2)), tuple(range(1, peers, 2))]
    firsts_of = list(range(0, peers, 4))
    pair = lambda m: (m, m + 2) if m + 2 < peers else (m,)
    teams = [pair(m + side) for m in firsts_of[::-1] for side in (1, 0)]
    back_teams = [pair(0)]
    for m in firsts_of[1:]:
        back_teams += [pair(m), pair(m + 1)]
    back_teams.append(pair(1))

    node_t = nodes.T
    edge_t = edges.T
    node_cot_t = node_cot.T
    edge_cot_t = edge_cot.T
    in_t = edge_in_weight.T
    send = send_nodes.reshape(rows, LANES)
    me = lax.axis_index("peer").astype(jnp.int32)[None]

    shards = gather_first(node_t)

    square = struct((feat, feat), bf16)
    vec, se_weight, re_weight, out_t, back_weight, edge_back, node_back, node_out_t, sr_weight = pl.pallas_call(
        prepare_kernel,
        out_shape=[
            struct((8, feat, LANES), f32), struct((feat, 2 * feat), bf16), square, square, square, square,
            struct((2 * feat, feat), bf16), square, struct((feat, 2 * feat), f32),
        ],
        name="prepare",
    )(
        in_t, edge_out_weight, node_in_weight.T, node_out_weight,
        *[v[None] for v in (edge_in_bias, edge_out_bias, edge_gain, edge_shift, node_in_bias, node_out_bias, node_gain, node_shift)],
    )

    wide = min(4096, per_peer)
    chunks = per_peer // wide
    sub = wide // LANES
    piece = min(2048, wide)

    def slab_of(masks):
        return pl.BlockSpec((feat, wide), lambda i, j, ref: (0, owner(masks, i, ref) * chunks + j))

    def rows_of(masks):
        return pl.BlockSpec((sub, LANES), lambda i, j, ref: (owner(masks, i, ref) * chunks + j, 0))

    def code_of(masks):
        return pl.BlockSpec((1, sub, LANES), lambda i, j, ref: (owner(masks, i, ref), j, 0))

    def kept_slab(place):
        return pl.BlockSpec((feat, wide), lambda i, j, ref: (0, (place + i) * chunks + j))

    own_slab = kept_slab(0)
    own_rows = pl.BlockSpec((sub, LANES), lambda i, j, ref: (i * chunks + j, 0))
    shard_spec = whole((feat, node_total))
    keep_spec = pl.BlockSpec(memory_space=pl.ANY)

    token = struct((8, LANES), f32)
    token_spec = whole((8, LANES))
    slab_shape = struct((feat, edge_total), bf16)
    shard_shape = struct((feat, node_total), bf16)
    picks, bases = [], []
    for masks in halves:
        count = len(masks)
        pick, base, gate = pl.pallas_call(
            functools.partial(sender_kernel, min(2048, wide), 0),
            grid_spec=pltpu.PrefetchScalarGridSpec(
                num_scalar_prefetch=1,
                grid=(count, chunks),
                in_specs=[shard_spec, rows_of(masks), slab_of(masks), whole((feat, 2 * feat)), whole((8, feat, LANES))],
                out_specs=[own_slab, own_slab, token_spec],
            ),
            out_shape=[struct((feat, count * per_peer), bf16), struct((feat, count * per_peer), f32), token],
            compiler_params=params(),
            name="sender",
        )(me, node_t, send, edge_t, se_weight, vec)
        if not picks:
            shards = gather_rest(shards, gate)
            send = tie(send, *[shards[m] for m in routed])
            live = jnp.arange(LANES, dtype=jnp.int32)[None, :] < tie(block_count, gate, *[shards[m] for m in [1] + routed])[:, None]
            code = slot_ids.reshape(block_total, LANES) + jnp.where(live, 0, LANES) + 2 * LANES * block_tile[:, None]
            code = lax.all_to_all(code, "peer", 0, 0, tiled=True)
            meta = jnp.concatenate([me, code[:, 0] // (2 * LANES)])
            code = (code & (2 * LANES - 1)).reshape(peers, blocks, LANES)
        picks.append(pick)
        bases.append(base)

    parts = {}
    chain = []
    saved = {}
    got = {}
    both = {}
    for masks in teams:
        count = len(masks)
        extra = len(chain)
        half_at, place = masks[0] % 2, masks[0] // 2
        base = bases[half_at]
        if masks == teams[-1] and len(teams) > 2:
            both = {m: join(parts, got, m) for m in routed if m in parts}
            base = tie(base, *both.values())
        result, act, slope, normed, inv, gate, *pieces = pl.pallas_call(
            functools.partial(forward_kernel, masks, blocks, piece, extra),
            grid_spec=pltpu.PrefetchScalarGridSpec(
                num_scalar_prefetch=1,
                grid=(count, chunks),
                in_specs=[code_of(masks), kept_slab(place), slab_of(masks), whole((feat, feat)), whole((feat, feat)), whole((8, feat, LANES))]
                + [shard_spec] * count
                + [keep_spec] * extra,
                out_specs=[slab_of(masks)] + [own_slab] * 3 + [own_rows, token_spec] + [shard_spec] * count,
                scratch_shapes=[pltpu.VMEM((feat, node_total), f32), pltpu.VMEM((feat, node_total), f32)],
            ),
            out_shape=[slab_shape] + [struct((feat, count * per_peer), bf16)] * 3
            + [struct((count * blocks, LANES), f32), token]
            + [shard_shape] * count,
            input_output_aliases={7 + count: 0} if extra else {},
            compiler_params=params(),
            name="forward",
        )(meta, code, base, edge_t, re_weight, out_t, vec, *[shards[m] for m in masks], *chain)
        chain = [result]
        saved[masks] = (normed, act, slope, inv)
        parts.update(zip(masks, pieces))
        if half_at:
            got.update({m - 1: swap(parts[m], 1) for m in masks})
    edge_result = result
    for m in routed:
        if m not in both:
            both[m] = join(parts, got, m)
    sums = [parts[0], got[0]] + [swap(both[m], m) for m in routed]

    node_result, node_base, back, node_pack = pl.pallas_call(
        functools.partial(node_kernel, len(sums)),
        out_shape=[
            struct((feat, node_total), bf16),
            struct((feat, node_total), f32),
            struct((feat, node_total), bf16),
            struct((feat + 8, 8 * feat), f32),
        ],
        compiler_params=params(),
        name="node",
    )(node_t, node_cot_t, node_in_weight.T, node_back, node_out_t, node_out_weight, vec, *sums)

    backs = gather_first(back)

    parts = {}
    got = {}
    chain = [node_pack]
    first_grads = {}
    for masks in back_teams:
        count = len(masks)
        extra = len(chain)
        half_at, place = masks[0] % 2, masks[0] // 2
        normed, act, slope, inv = saved[masks]
        *outs, = pl.pallas_call(
            functools.partial(backward_kernel, masks, blocks, piece, extra),
            grid_spec=pltpu.PrefetchScalarGridSpec(
                num_scalar_prefetch=1,
                grid=(count, chunks),
                in_specs=[code_of(masks), slab_of(masks)] + [own_slab] * 3 + [own_rows, slab_of(masks), kept_slab(place)]
                + [whole((feat, feat)), whole((feat, feat)), whole((8, feat, LANES))]
                + [shard_spec] * (2 * count)
                + [whole((feat + 8, 8 * feat))]
                + [keep_spec] * (extra - 1),
                out_specs=[slab_of(masks), own_slab, whole((feat + 8, 8 * feat)), token_spec] + [shard_spec] * count,
                scratch_shapes=[
                    pltpu.VMEM((feat, node_total), f32),
                    pltpu.VMEM((feat, node_total), f32),
                    pltpu.VMEM((feat, 2 * feat), f32),
                    pltpu.VMEM((feat, feat), f32),
                    pltpu.VMEM((feat, feat), f32),
                    pltpu.VMEM((4, feat, LANES), f32),
                ],
            ),
            out_shape=[
                struct((feat, edge_total), f32),
                struct((feat, count * per_peer), bf16),
                struct((feat + 8, 8 * feat), f32),
                token,
            ]
            + [shard_shape] * count,
            input_output_aliases={13 + 2 * count: 0} if extra > 1 else {},
            compiler_params=params(),
            name="backward",
        )(
            meta, code, edge_cot_t, normed, act, slope, inv, edge_t, picks[half_at], back_weight, edge_back, vec,
            *[backs[m] for m in masks], *[shards[m] for m in masks], *chain,
        )
        edge_grad, first_grads[masks], edge_pack, gate, *pieces = outs
        chain = [edge_pack, edge_grad]
        parts.update(zip(masks, pieces))
        if half_at:
            got.update({m - 1: swap(parts[m], 1) for m in masks})
        if masks == back_teams[0]:
            backs = gather_rest(backs, gate)

    near_pack = swap(edge_pack, 1)
    late = [m for m in routed if m + 1 in back_teams[-1]]
    early = [m for m in routed if m not in late]
    both = {}
    marks = []
    if early:
        marks = lax.optimization_barrier([got[m] for m in early])
        both = {m: join(parts, {m: value}, m) for m, value in zip(early, marks)}
        marks = [both[m] for m in early]
    there = {m: swap(both[m], m) for m in early}
    edge_pack = edge_pack + tie(near_pack, *marks)
    far = swap(edge_pack, peers // 2) if peers > 2 else None

    sum_wide = min(4096, per_peer)
    sum_chunks = per_peer // sum_wide

    def add_sent(masks_list, hold):
        masks = [m for masks in masks_list for m in masks]
        arrays = [first_grads[masks] for masks in masks_list]
        if hold:
            arrays[0] = tie(arrays[0], *hold)
        spans = [a.shape[1] // sum_wide for a in arrays]
        starts = [sum(spans[:k]) for k in range(len(spans))]

        def send_at(i, ref):
            step = i // sum_chunks
            mask = masks[0]
            for k in range(1, len(masks)):
                mask = jnp.where(step == k, masks[k], mask)
            return ((ref[0] ^ mask) * sum_chunks + i % sum_chunks, 0)

        return pl.pallas_call(
            functools.partial(sender_sum_kernel, tuple(starts)),
            grid_spec=pltpu.PrefetchScalarGridSpec(
                num_scalar_prefetch=1,
                grid=(len(masks) * sum_chunks,),
                in_specs=[pl.BlockSpec((sum_wide // LANES, LANES), send_at)]
                + [
                    pl.BlockSpec((feat, sum_wide), lambda i, ref, start=start, span=span: (0, jnp.clip(i - start, 0, span - 1)))
                    for start, span in zip(starts, spans)
                ],
                out_specs=[shard_spec, token_spec],
                scratch_shapes=[pltpu.VMEM((node_total // WIDE * feat, WIDE), f32), pltpu.VMEM((feat, sum_wide), bf16)],
            ),
            out_shape=[struct((feat, node_total), f32), token],
            compiler_params=params(),
            name="sender_sum",
        )(me, send, *arrays)

    sent_first, gate = add_sent(back_teams[:-1], marks)
    for m in late:
        both[m] = join(parts, {m: tie(got[m], gate)}, m)
        there[m] = swap(both[m], m)
    if far is not None:
        edge_pack = edge_pack + tie(far, gate)
        edge_pack = add_groups(tie(edge_pack, got[0]))
        mask = 2
        while mask < peers // 2:
            edge_pack = edge_pack + swap(edge_pack, mask)
            mask *= 2
    sent_last, gate = add_sent(back_teams[-1:], [there[m] for m in early])
    sent = [sent_first, sent_last]
    both_packs = tie(edge_pack, gate)
    sums = [parts[0], got[0]] + [there[m] for m in routed]

    vec_out = struct((1, feat), f32)
    node_grad, e1, b1, e2, b2, g1, s1, n1, c1, n2, c2, g2, s2 = pl.pallas_call(
        functools.partial(finish_kernel, len(sent), len(sums)),
        out_shape=[
            struct((feat, node_total), f32),
            struct((feat, 3 * feat), f32), vec_out, struct((feat, feat), f32), vec_out, vec_out, vec_out,
            struct((feat, 2 * feat), f32), vec_out, struct((feat, feat), f32), vec_out, vec_out, vec_out,
        ],
        compiler_params=params(),
        name="finish",
    )(node_base, sr_weight, both_packs, *sent, *sums)

    def flat(row):
        return row.reshape(feat)

    return (
        node_result.T, edge_result.T, node_grad.T, edge_grad.T,
        e1.T, flat(b1), e2, flat(b2), flat(g1), flat(s1),
        n1.T, flat(c1), n2, flat(c2), flat(g2), flat(s2),
    )


def solution(mesh):
    split = P(("grp", "peer"), None)
    line = P(("grp", "peer"))
    one = P()
    return jax.shard_map(
        functools.partial(per_device, mesh.shape["grp"], mesh.shape["peer"]),
        mesh=mesh,
        in_specs=(split, split, line, line, line, line) + (one,) * 12 + (split, split),
        out_specs=(split, split, split, split) + (one,) * 12,
        check_vma=False,
    )
```
